32 devices in a mesh: dp: 1 (over z), ep: 32 (over x, y, core).
Axes of the slice: x: 4, y: 4, z: 1, core: 2. Of those that a mesh axis runs over, the one named last changes fastest.
The devices are a block of a 4x4x8 slice.
Arguments:
- x: bfloat16 [1, 32, 256, 2048], P('dp', 'ep')
- expert: int32 [1, 32, 256, 6], P('dp', 'ep')
- slot: int32 [1, 32, 256, 6], P('dp', 'ep')
- gate: float32 [1, 32, 256, 6], P('dp', 'ep')
- w_gate: bfloat16 [64, 2048, 1408], P('ep')
- w_up: bfloat16 [64, 2048, 1408], P('ep')
- w_down: bfloat16 [64, 1408, 2048], P('ep')
- s_gate: bfloat16 [2048, 2816], replicated
- s_up: bfloat16 [2048, 2816], replicated
- s_down: bfloat16 [2816, 2048], replicated
Outputs:
- y: bfloat16 [1, 32, 256, 2048], P('dp', 'ep')
All inputs are finite; a program needn't handle non-finite values.
Results may differ from the reference program's by a relative error of at most 0.009.
Values are sent between devices in bfloat16 or wider.
A program may use at most 768 MiB of HBM per device.

```python
import jax
import jax.numpy as jnp

MEMBERS = 32
TOKENS = 256
D = 2048
FF = 1408
TOP = 6
EXPERTS = 64
SHARED_FF = 2816
SLOTS = 5 * TOKENS * TOP // (4 * EXPERTS)


def setup_inputs(seed: int = 0, part: int = 0) -> dict:
    own, k1, k2, k3, k4, k5, k6 = jax.random.split(jax.random.key(seed), 7)
    kx, ke, kl, kg = jax.random.split(jax.random.fold_in(own, part), 4)
    devices = (1, MEMBERS)
    place = jax.random.permutation(kl, jnp.arange(EXPERTS, dtype=jnp.uint32))
    slow = ((EXPERTS + (9 * place) % EXPERTS) << ((9 * place) // EXPERTS)) // EXPERTS
    wait = (jax.random.bits(ke, (*devices, TOKENS, EXPERTS), jnp.uint32) >> 10) * slow
    expert = jnp.argsort(wait, axis=-1)[..., :TOP].astype(jnp.int32)
    chosen = jax.nn.one_hot(expert, EXPERTS, dtype=jnp.int32)
    in_line = jnp.cumsum(chosen.reshape(*devices, TOKENS * TOP, EXPERTS), axis=2) - 1
    slot = jnp.sum(in_line.reshape(chosen.shape) * chosen, axis=-1)

    def one(key, rows, columns):
        return (jax.random.normal(key, (rows, columns), jnp.float32) * rows**-0.5).astype(jnp.bfloat16)

    def weights(key, rows, columns):
        return jax.lax.map(lambda k: one(k, rows, columns), jax.random.split(key, EXPERTS))

    return {
        "x": jax.random.normal(kx, (*devices, TOKENS, D), jnp.float32).astype(jnp.bfloat16),
        "expert": expert,
        "slot": slot,
        "gate": jax.nn.softmax(jax.random.normal(kg, expert.shape, jnp.float32)),
        "w_gate": weights(k1, D, FF),
        "w_up": weights(k2, D, FF),
        "w_down": weights(k3, FF, D),
        "s_gate": one(k4, D, SHARED_FF),
        "s_up": one(k5, D, SHARED_FF),
        "s_down": one(k6, SHARED_FF, D),
    }


def einsum(form, a, b):
    return jnp.einsum(form, a.astype(jnp.float32), b.astype(jnp.float32))


def for_all(x, s_gate, s_up, s_down):
    h = jax.nn.silu(einsum("...d,df->...f", x, s_gate)) * einsum("...d,df->...f", x, s_up)
    return einsum("...f,fd->...d", h.astype(jnp.bfloat16), s_down)


def reference(x, expert, slot, gate, w_gate, w_up, w_down, s_gate, s_up, s_down):
    to_expert = jax.nn.one_hot(expert, EXPERTS, dtype=jnp.bfloat16)
    to_slot = jax.nn.one_hot(slot, SLOTS, dtype=jnp.bfloat16)
    weighted = to_expert * gate[..., None].astype(jnp.bfloat16)
    dispatch = einsum("abtke,abtkc->abtec", to_expert, to_slot).astype(jnp.bfloat16)
    combine = einsum("abtke,abtkc->abtec", weighted, to_slot).astype(jnp.bfloat16)
    z = einsum("abtec,abtd->aebcd", dispatch, x).astype(jnp.bfloat16)
    h = jax.nn.silu(einsum("aebcd,edf->aebcf", z, w_gate))
    h = (h * einsum("aebcd,edf->aebcf", z, w_up)).astype(jnp.bfloat16)
    out = einsum("aebcf,efd->aebcd", h, w_down).astype(jnp.bfloat16)
    y = einsum("abtec,aebcd->abtd", combine, out)
    return (y + for_all(x, s_gate, s_up, s_down)).astype(jnp.bfloat16)
```

```python
import contextlib
import functools
import math

import jax
import jax.numpy as jnp
from jax import lax
from jax.experimental import pallas as pl
from jax.experimental.pallas import tpu as pltpu
from jax.sharding import PartitionSpec as P

MESH = pl.DeviceIdType.MESH
OFFSETS = 4
HERE, ON, BACK, FAR = range(OFFSETS)
SAME, OTHER = range(2)
UNITS = ((HERE, SAME), (HERE, OTHER), (ON, SAME), (BACK, SAME), (ON, OTHER), (BACK, OTHER), (FAR, SAME), (FAR, OTHER))
LANE = 128
WIDE = 2 * LANE
BUFFERS = 6
COPIES = 33
BF16, F32 = jnp.bfloat16, jnp.float32
scope = contextlib.nullcontext


def dot(a, b):
    return jnp.dot(a, b, preferred_element_type=F32)


def swiglu(both):
    g, u = both[:, :LANE], both[:, LANE:]
    return (g * jax.nn.sigmoid(g) * u).astype(BF16)


def kernel(side, slots, x_hbm, expert_ref, slot_ref, gate_ref, wg, wu, wd, sg, su, sd, y_ref,
           xg, mg, column, onehot, combine, sent, fwd, z, r, fwdb, h, w, part, near, rfar, rn, ysh,
           in_sem, w_sem, send_sem, recv_sem):
    tokens, d = x_hbm.shape
    per, _, ff = wg.shape
    group = OFFSETS * slots
    unit = per * group
    rows = group + (-group) % 16
    last = unit - rows
    half = tokens // 2
    full = unit + (-unit) % LANE
    units = len(UNITS)
    total = units * full
    index = {u: k for k, u in enumerate(UNITS)}

    me = lax.axis_index("ep")
    core, chip = lax.rem(me, 2), lax.div(me, 2)
    py, px = lax.rem(chip, side), lax.div(chip, side)
    pa, pb = px + (py - px) * core, py + (px - py) * core
    sa, sb = 2 * side - (2 * side - 2) * core, 2 + (2 * side - 2) * core

    def at(da, db, other):
        a, b = lax.rem(pa + da + side, side), lax.rem(pb + db + side, side)
        return sa * a + sb * b + (1 - core if other else core)

    def copy(i, src, dst, to):
        return pltpu.make_async_remote_copy(
            src_ref=src, dst_ref=dst, send_sem=send_sem.at[i], recv_sem=recv_sem.at[i],
            device_id={"ep": to}, device_id_type=MESH)

    lo, hi, body = pl.ds(0, half), pl.ds(half, half), pl.ds(0, unit)
    c = {}

    def link(name, src, dst, to):
        c[name] = copy(len(c), src, dst, to)

    def back(i, j):
        return r.at[index[i, j], body]

    for i, way, first, second in ((ON, 1, lo, hi), (BACK, -1, hi, lo)):
        link(("x", i, 0), xg.at[HERE, first], xg.at[i, first], at(way, 0, SAME))
        link(("x", i, 1), xg.at[HERE, second], xg.at[i, second], at(way, 0, SAME))
        link(("m", i), mg.at[HERE], mg.at[i], at(way, 0, SAME))
        link(("xx", i), xg.at[i, first], xg.at[FAR, first], at(way, 0, SAME))
    link("mm", mg.at[ON], mg.at[FAR], at(1, 0, SAME))
    link(("z", HERE, OTHER), sent.at[HERE, OTHER], z.at[OTHER, HERE], at(0, 0, OTHER))
    link(("r", HERE, OTHER), z.at[OTHER, HERE], back(HERE, OTHER), at(0, 0, OTHER))
    for i, way in ((ON, 1), (BACK, -1)):
        for j in (SAME, OTHER):
            link(("z", i, j), sent.at[i, j], z.at[j, i], at(0, way, j))
        link(("r", i, SAME), z.at[SAME, i], back(i, SAME), at(0, -way, SAME))
        link(("r", i, OTHER), z.at[OTHER, i], back(i, OTHER), at(-way, 0, OTHER))
    for j, way in ((SAME, 1), (OTHER, -1)):
        link(("f", j), sent.at[FAR, j], fwd.at[j], at(0, way, SAME))
        link(("z", FAR, j), fwd.at[j], z.at[j, FAR], at(0, way, j))
        link(("r", FAR, j), fwdb.at[j], back(FAR, j), at(0, -way, SAME))
    link(("g", SAME), z.at[SAME, FAR], fwdb.at[SAME], at(0, -1, SAME))
    link(("g", OTHER), z.at[OTHER, FAR], fwdb.at[OTHER], at(1, 0, OTHER))
    for k, way, first, second in ((0, 1, lo, hi), (1, -1, hi, lo)):
        link(("pp", k), part.at[2, first], rfar.at[k], at(way, 0, SAME))
        link(("p", k, 0), part.at[k, second], rn.at[k, second], at(way, 0, SAME))
        link(("p", k, 1), part.at[k, first], rn.at[k, first], at(way, 0, SAME))
    assert len(c) == COPIES

    def start(*which):
        for i in which:
            c[i].start()

    def arrived(*which):
        for i in which:
            c[i].wait_recv()

    n_up, n_down, passes = ff // LANE, d // WIDE, 5
    n_tiles = n_up + n_down
    ahead = BUFFERS - 2
    assert per == 2 and n_up % 2 == 1 and n_down % 2 == 0

    def slot_of(p, t):
        return lax.rem(p * n_tiles + t, BUFFERS)

    def up_tile(p, t):
        slot = slot_of(p, t)
        out = []
        for e in range(per):
            for k, (shared, own) in enumerate(((sg, wg), (su, wu))):
                if p == 0:
                    src = shared.at[:, pl.ds(pl.multiple_of(e * ff + t * LANE, LANE), LANE)]
                else:
                    src = own.at[e, :, pl.ds(pl.multiple_of(t * LANE, LANE), LANE)]
                out.append(pltpu.make_async_copy(
                    src, w.at[slot, e, :, pl.ds(k * LANE, LANE)], w_sem.at[slot, len(out)]))
        return out

    def down_tile(p, t):
        slot = slot_of(p, t)
        cols = pl.ds(pl.multiple_of((t - n_up) * WIDE, WIDE), WIDE)
        out = []
        for e in range(per):
            src = sd.at[pl.ds(e * ff, ff), cols] if p == 0 else wd.at[e, :, cols]
            out.append(pltpu.make_async_copy(src, w.at[slot, e, pl.ds(0, ff), :], w_sem.at[slot, len(out)]))
        return out

    def go(copies):
        for one in copies:
            one.start()

    def done(copies):
        for one in copies:
            one.wait()

    def fetch_in_up(p, q):
        @pl.when(q < n_up)
        def _():
            go(up_tile(p, q))

        @pl.when(q >= n_up)
        def _():
            go(down_tile(p, q))

    def fetch_in_down(p, q):
        @pl.when(q < n_tiles)
        def _():
            go(down_tile(p, q))

        if p + 1 < passes:
            @pl.when(q >= n_tiles)
            def _():
                go(up_tile(p + 1, q - n_tiles))

    def ups(p, lhs):
        def some(ts):
            for t in ts:
                done(up_tile(p, t))
            for t in ts:
                fetch_in_up(p, t + ahead)
            for t in ts:
                for e in range(per):
                    v = swiglu(dot(lhs(e), w[slot_of(p, t), e]))
                    h[e, :, pl.ds(pl.multiple_of(t * LANE, LANE), LANE)] = v

        @pl.loop(0, n_up // 2)
        def _(i):
            some((2 * i, 2 * i + 1))

        some((jnp.int32(n_up - 1),))

    def downs(p, store):
        @pl.loop(0, n_down // 2)
        def _(i):
            ts = (n_up + 2 * i, n_up + 2 * i + 1)
            for t in ts:
                done(down_tile(p, t))
            for t in ts:
                fetch_in_down(p, t + ahead)
            for t in ts:
                cols = pl.ds(pl.multiple_of((t - n_up) * WIDE, WIDE), WIDE)
                store(cols, *(dot(h[e], w[slot_of(p, t), e, pl.ds(0, ff), :]) for e in range(per)))

    def expert_ups(p, a, b):
        def lhs(e):
            these = pl.ds(e * last, rows)
            return jnp.concatenate([z[*a, these, :], z[*b, these, :]], axis=0)
        ups(p, lhs)

    def expert_downs(p, a, b):
        def store(cols, first, second):
            for k, ref in enumerate((a, b)):
                v, u = (o[k * rows:(k + 1) * rows] for o in (first, second))
                row = lax.broadcasted_iota(jnp.int32, (rows - last, WIDE), 0)
                edge = jnp.where(row < group - last, v[last:], u[:rows - last])
                ref[pl.ds(0, last), cols] = v[:last].astype(BF16)
                ref[pl.ds(last, rows - last), cols] = edge.astype(BF16)
                ref[pl.ds(rows, last), cols] = u[rows - last:].astype(BF16)
        downs(p, store)

    def routing():
        def place(to, here):
            away = lax.rem(to - here + side, side)
            return away ^ lax.shift_right_logical(away, 1)

        tos, spots, numbers = [], [], []
        number = lax.broadcasted_iota(jnp.int32, (1, tokens), 1).astype(F32) + 1.0
        n_to = OFFSETS * units
        for k in range(expert_ref.shape[0]):
            expert, slot = expert_ref[k], slot_ref[k]
            device, e = lax.div(expert, per), lax.rem(expert, per)
            other = lax.rem(device, 2) ^ core
            chip_to = lax.div(device, 2)
            ty, tx = lax.rem(chip_to, side), lax.div(chip_to, side)
            ta, tb = tx + (ty - tx) * core, ty + (tx - ty) * core
            oa, ob = place(ta, pa), place(tb, pb)
            u = jnp.where(ob == HERE, other, jnp.where(ob == FAR, index[FAR, SAME] + other, ob + 1 + 2 * other))
            to = u * OFFSETS + oa
            spot = jnp.where(slot < slots, (e * OFFSETS + oa) * slots + slot, -1)
            tos.append(jnp.where(lax.broadcasted_iota(jnp.int32, (n_to, tokens), 0) == to, 1.0, 0.0).astype(BF16))
            hit = lax.broadcasted_iota(jnp.int32, (full, tokens), 0) == spot
            spots.append(jnp.where(hit, number, 0.0).astype(BF16))
            numbers.append(jnp.where(hit, gate_ref[k], 0.0).astype(BF16))
        a = jnp.concatenate(tos, axis=1)
        for base, b in ((0, spots), (OFFSETS, numbers)):
            found = lax.dot_general(a, jnp.concatenate(b, axis=1), (((1,), (1,)), ((), ())),
                                    preferred_element_type=F32)
            for u in range(units):
                mg[HERE, pl.ds(base, OFFSETS), pl.ds(u * full, full)] = found[u * OFFSETS:(u + 1) * OFFSETS]

    x_in = pltpu.make_async_copy(x_hbm, xg.at[HERE], in_sem.at[0])
    with scope("enter"):
        x_in.start()
        for t in range(ahead):
            go(up_tile(0, t))
        barrier = pltpu.get_barrier_semaphore()
        peers = [at(da, db, j) for da, db in ((1, 0), (-1, 0), (0, 1), (0, -1)) for j in (SAME, OTHER)]
        peers.append(at(0, 0, OTHER))
        for peer in peers:
            pl.semaphore_signal(barrier, inc=1, device_id={"ep": peer}, device_id_type=MESH)
    with scope("routing"):
        routing()
        if full > unit:
            r[:, pl.ds(unit, full - unit), :] = jnp.zeros((units, full - unit, d), BF16)
    with scope("x_in"):
        x_in.wait()
        pl.semaphore_wait(barrier, len(peers))
        for k in range(2):
            start(("x", ON, k), ("x", BACK, k))
        start(("m", ON), ("m", BACK))

    with scope("shared_up"):
        ups(0, lambda e: xg[HERE])

    def shared_store(cols, first, second):
        ysh[:, cols] = first + second

    with scope("x_wait"):
        for i in (ON, BACK):
            arrived(("x", i, 0))
            start(("xx", i))
    with scope("shared_down"):
        downs(0, shared_store)
    with scope("xx_wait"):
        for i in (ON, BACK):
            arrived(("x", i, 1), ("m", i))
        start("mm")
        arrived(("xx", ON), ("xx", BACK), "mm")

    def table(s, base=0):
        return mg[s, s + base:s + base + 1, :]

    with scope("tables"):
        merged = jnp.zeros(mg.shape[1:], F32)
        row = lax.broadcasted_iota(jnp.int32, merged.shape, 0)
        for s in range(OFFSETS):
            merged = jnp.where(row == s, mg[s], merged)
        column[...] = jnp.transpose(merged)

    step = min(d, 8 * LANE)

    def gather(i, j, out):
        begin = index[i, j] * full
        lane = lax.broadcasted_iota(jnp.int32, (unit, tokens), 1).astype(F32) + 1.0
        for s in range(OFFSETS):
            token = column[pl.ds(begin, unit), s:s + 1]
            onehot[:, pl.ds(s * tokens, tokens)] = jnp.where(lane == token, 1.0, 0.0).astype(BF16)

        @pl.loop(0, d // step)
        def _(k):
            cols = pl.ds(pl.multiple_of(k * step, step), step)
            out[:, cols] = dot(onehot[...], xg[:, :, cols].reshape(OFFSETS * tokens, step)).astype(BF16)

    def gather_and_send(i, j):
        with scope("gather"):
            gather(i, j, sent.at[i, j])
        start(("f", j) if i == FAR else ("z", i, j))

    gather_and_send(FAR, SAME)
    gather_and_send(FAR, OTHER)
    gather_and_send(ON, SAME)
    gather_and_send(BACK, SAME)
    gather_and_send(HERE, OTHER)
    with scope("gather"):
        gather(HERE, SAME, z.at[SAME, HERE])
        gather(ON, OTHER, sent.at[ON, OTHER])
        gather(BACK, OTHER, sent.at[BACK, OTHER])
    with scope("wait_f"):
        for j in (SAME, OTHER):
            arrived(("f", j))
            start(("z", FAR, j))
    start(("z", ON, OTHER), ("z", BACK, OTHER))

    with scope("wait_here"):
        arrived(("z", HERE, OTHER))
    with scope("ffn_here"):
        expert_ups(1, (SAME, HERE), (OTHER, HERE))
        expert_downs(1, r.at[index[HERE, SAME]], z.at[OTHER, HERE])
    start(("r", HERE, OTHER))
    with scope("wait_same"):
        arrived(("z", ON, SAME), ("z", BACK, SAME))
    with scope("ffn_same"):
        expert_ups(2, (SAME, ON), (SAME, BACK))
        expert_downs(2, z.at[SAME, ON], z.at[SAME, BACK])
    start(("r", ON, SAME), ("r", BACK, SAME))
    with scope("wait_far"):
        arrived(("z", FAR, SAME), ("z", FAR, OTHER))
    with scope("ffn_far"):
        expert_ups(3, (SAME, FAR), (OTHER, FAR))
        expert_downs(3, z.at[SAME, FAR], z.at[OTHER, FAR])
    start(("g", SAME), ("g", OTHER))
    with scope("wait_other"):
        arrived(("z", ON, OTHER), ("z", BACK, OTHER))
    with scope("ffn_other_up"):
        expert_ups(4, (OTHER, ON), (OTHER, BACK))
    with scope("ffn_other_down"):
        expert_downs(4, z.at[OTHER, ON], z.at[OTHER, BACK])
    start(("r", ON, OTHER), ("r", BACK, OTHER))
    with scope("wait_g"):
        for j in (SAME, OTHER):
            arrived(("g", j))
            start(("r", FAR, j))
    with scope("wait_r_near"):
        arrived(*(("r", i, j) for i, j in UNITS[1:] if i != FAR))
    with scope("wait_r_far"):
        arrived(("r", FAR, SAME), ("r", FAR, OTHER))

    def add_up(s, store):
        token = lax.broadcasted_iota(jnp.int32, (tokens, total), 0).astype(F32) + 1.0
        combine[...] = jnp.where(token == table(s), table(s, OFFSETS), 0.0).astype(BF16)

        @pl.loop(0, d // step)
        def _(k):
            cols = pl.ds(pl.multiple_of(k * step, step), step)
            store(cols, dot(combine[...], r[:, :, cols].reshape(total, step)))

    def keep_far(cols, o):
        part[2, :, cols] = o.astype(BF16)

    def keep_next(cols, o):
        near[0, :, cols] = o[:half]
        part[0, hi, cols] = o[half:].astype(BF16)

    def keep_back(cols, o):
        near[1, :, cols] = o[half:]
        part[1, lo, cols] = o[:half].astype(BF16)

    def keep_own(cols, o):
        ysh[:, cols] = ysh[:, cols] + o

    with scope("sum_far"):
        add_up(FAR, keep_far)
    start(("pp", 0), ("pp", 1))
    with scope("sum_near"):
        add_up(BACK, keep_next)
        start(("p", 0, 0))
        add_up(ON, keep_back)
        start(("p", 1, 0))
    with scope("wait_pp"):
        for k, first in ((0, lo), (1, hi)):
            arrived(("pp", k))
            part[k, first, :] = (near[k] + rfar[k].astype(F32)).astype(BF16)
            start(("p", k, 1))
    with scope("sum_own"):
        add_up(HERE, keep_own)
    with scope("wait_p"):
        arrived(*(("p", k, v) for k in range(2) for v in range(2)))
    with scope("leave"):
        y_ref[...] = (ysh[...] + (rn[0].astype(F32) + rn[1].astype(F32))).astype(y_ref.dtype)
        for one in c.values():
            one.wait_send()


def solution(mesh):
    side = math.isqrt(mesh.shape["ep"] // 2)
    assert side == OFFSETS

    def local(x, expert, slot, gate, w_gate, w_up, w_down, s_gate, s_up, s_down):
        tokens, d = x.shape[2:]
        top = expert.shape[3]
        per, _, ff = w_gate.shape
        experts = per * mesh.shape["ep"]
        slots = 5 * tokens * top // (4 * experts)
        unit = per * OFFSETS * slots
        full = unit + (-unit) % LANE
        half, units = tokens // 2, len(UNITS)
        choices = (v.reshape(tokens, top).T.reshape(top, 1, tokens) for v in (expert, slot, gate))
        anywhere, vmem = pl.BlockSpec(memory_space=pl.ANY), pl.BlockSpec(memory_space=pltpu.VMEM)
        y = pl.pallas_call(
            functools.partial(kernel, side, slots),
            out_shape=jax.ShapeDtypeStruct((tokens, d), x.dtype),
            in_specs=[anywhere] + [vmem] * 3 + [anywhere] * 6,
            out_specs=vmem,
            scratch_shapes=[
                pltpu.VMEM((OFFSETS, tokens, d), BF16),
                pltpu.VMEM((OFFSETS, 2 * OFFSETS, units * full), F32),
                pltpu.VMEM((units * full, 2 * OFFSETS), F32),
                pltpu.VMEM((unit, OFFSETS * tokens), BF16),
                pltpu.VMEM((tokens, units * full), BF16),
                pltpu.VMEM((OFFSETS, 2, unit, d), BF16),
                pltpu.VMEM((2, unit, d), BF16),
                pltpu.VMEM((2, OFFSETS, unit, d), BF16),
                pltpu.VMEM((units, full, d), BF16),
                pltpu.VMEM((2, unit, d), BF16),
                pltpu.VMEM((per, 2 * (unit // per + 8), ff), BF16),
                pltpu.VMEM((BUFFERS, per, d, WIDE), BF16),
                pltpu.VMEM((3, tokens, d), BF16),
                pltpu.VMEM((2, half, d), F32),
                pltpu.VMEM((2, half, d), BF16),
                pltpu.VMEM((2, tokens, d), BF16),
                pltpu.VMEM((tokens, d), F32),
                pltpu.SemaphoreType.DMA((1,)),
                pltpu.SemaphoreType.DMA((BUFFERS, 4)),
                pltpu.SemaphoreType.DMA((COPIES,)),
                pltpu.SemaphoreType.DMA((COPIES,)),
            ],
            compiler_params=pltpu.CompilerParams(
                collective_id=0, has_side_effects=True, vmem_limit_bytes=67_000_000),
            name="moe",
        )(x.reshape(tokens, d), *choices, w_gate, w_up, w_down, s_gate, s_up, s_down)
        return y.reshape(x.shape)

    spread, held, whole = P("dp", "ep", None, None), P("ep", None, None), P(None, None)
    return jax.shard_map(
        local, mesh=mesh, in_specs=(spread,) * 4 + (held,) * 3 + (whole,) * 3, out_specs=spread, check_vma=False)
```

```python
import contextlib
import functools
import math

import jax
import jax.numpy as jnp
from jax import lax
from jax.experimental import pallas as pl
from jax.experimental.pallas import tpu as pltpu
from jax.sharding import PartitionSpec as P

MESH = pl.DeviceIdType.MESH
OFFSETS = 4
HERE, ON, BACK, FAR = range(OFFSETS)
SAME, OTHER = range(2)
UNITS = ((HERE, SAME), (HERE, OTHER), (ON, SAME), (BACK, SAME), (ON, OTHER), (BACK, OTHER), (FAR, SAME), (FAR, OTHER))
LANE = 128
WIDE = 2 * LANE
BUFFERS = 6
COPIES = 34
BF16, F32 = jnp.bfloat16, jnp.float32
scope = contextlib.nullcontext


def dot(a, b):
    return jnp.dot(a, b, preferred_element_type=F32)


def swiglu(both):
    g, u = both[:, :LANE], both[:, LANE:]
    return (g * jax.nn.sigmoid(g) * u).astype(BF16)


def kernel(side, slots, x_hbm, expert_hbm, slot_hbm, gate_hbm, wg, wu, wd, sg, su, sd, y_ref,
           expert_ref, slot_ref, gate_ref, xg, mg, column, onehot, combine, sent, fwd, z, r, fwdb, h, w, part, near, rfar, rn, ysh,
           in_sem, w_sem, send_sem, recv_sem):
    tokens, d = x_hbm.shape
    per, _, ff = wg.shape
    group = OFFSETS * slots
    unit = per * group
    rows = group + (-group) % 16
    last = unit - rows
    half = tokens // 2
    full = unit + (-unit) % LANE
    units = len(UNITS)
    total = units * full
    index = {u: k for k, u in enumerate(UNITS)}

    me = lax.axis_index("ep")
    core, chip = lax.rem(me, 2), lax.div(me, 2)
    py, px = lax.rem(chip, side), lax.div(chip, side)
    pa, pb = px + (py - px) * core, py + (px - py) * core
    sa, sb = 2 * side - (2 * side - 2) * core, 2 + (2 * side - 2) * core

    def at(da, db, other):
        a, b = lax.rem(pa + da + side, side), lax.rem(pb + db + side, side)
        return sa * a + sb * b + (1 - core if other else core)

    def copy(i, src, dst, to):
        return pltpu.make_async_remote_copy(
            src_ref=src, dst_ref=dst, send_sem=send_sem.at[i], recv_sem=recv_sem.at[i],
            device_id={"ep": to}, device_id_type=MESH)

    lo, hi, body = pl.ds(0, half), pl.ds(half, half), pl.ds(0, unit)
    c = {}

    def link(name, src, dst, to):
        c[name] = copy(len(c), src, dst, to)

    def back(i, j):
        return r.at[index[i, j], body]

    for i, way, first, second in ((ON, 1, lo, hi), (BACK, -1, hi, lo)):
        link(("x", i, 0), xg.at[HERE, first], xg.at[i, first], at(way, 0, SAME))
        link(("x", i, 1), xg.at[HERE, second], xg.at[i, second], at(way, 0, SAME))
        link(("m", i), mg.at[HERE, i], mg.at[i, i], at(way, 0, SAME))
        link(("xx", i), xg.at[i, first], xg.at[FAR, first], at(way, 0, SAME))
    link(("m", FAR), mg.at[HERE, FAR], mg.at[ON, FAR], at(1, 0, SAME))
    link("mm", mg.at[ON, FAR], mg.at[FAR, FAR], at(1, 0, SAME))
    link(("z", HERE, OTHER), sent.at[HERE, OTHER], z.at[OTHER, HERE], at(0, 0, OTHER))
    link(("r", HERE, OTHER), z.at[OTHER, HERE], back(HERE, OTHER), at(0, 0, OTHER))
    for i, way in ((ON, 1), (BACK, -1)):
        for j in (SAME, OTHER):
            link(("z", i, j), sent.at[i, j], z.at[j, i], at(0, way, j))
        link(("r", i, SAME), z.at[SAME, i], back(i, SAME), at(0, -way, SAME))
        link(("r", i, OTHER), z.at[OTHER, i], back(i, OTHER), at(-way, 0, OTHER))
    for j, way in ((SAME, 1), (OTHER, -1)):
        link(("f", j), sent.at[FAR, j], fwd.at[j], at(0, way, SAME))
        link(("z", FAR, j), fwd.at[j], z.at[j, FAR], at(0, way, j))
        link(("r", FAR, j), fwdb.at[j], back(FAR, j), at(0, -way, SAME))
    link(("g", SAME), z.at[SAME, FAR], fwdb.at[SAME], at(0, -1, SAME))
    link(("g", OTHER), z.at[OTHER, FAR], fwdb.at[OTHER], at(1, 0, OTHER))
    for k, way, first, second in ((0, 1, lo, hi), (1, -1, hi, lo)):
        link(("pp", k), part.at[2, first], rfar.at[k], at(way, 0, SAME))
        link(("p", k, 0), part.at[k, second], rn.at[k, second], at(way, 0, SAME))
        link(("p", k, 1), part.at[k, first], rn.at[k, first], at(way, 0, SAME))
    assert len(c) == COPIES

    def start(*which):
        for i in which:
            c[i].start()

    def arrived(*which):
        for i in which:
            c[i].wait_recv()

    n_up, n_down, passes = ff // LANE, d // WIDE, 5
    n_tiles = n_up + n_down
    ahead = BUFFERS - 2
    assert per == 2 and n_up % 2 == 1 and n_down % 2 == 0

    def slot_of(p, t):
        return lax.rem(p * n_tiles + t, BUFFERS)

    def up_tile(p, t):
        slot = slot_of(p, t)
        out = []
        for e in range(per):
            for k, (shared, own) in enumerate(((sg, wg), (su, wu))):
                if p == 0:
                    src = shared.at[:, pl.ds(pl.multiple_of(e * ff + t * LANE, LANE), LANE)]
                else:
                    src = own.at[e, :, pl.ds(pl.multiple_of(t * LANE, LANE), LANE)]
                out.append(pltpu.make_async_copy(
                    src, w.at[slot, e, :, pl.ds(k * LANE, LANE)], w_sem.at[slot, len(out)]))
        return out

    def down_tile(p, t):
        slot = slot_of(p, t)
        cols = pl.ds(pl.multiple_of((t - n_up) * WIDE, WIDE), WIDE)
        out = []
        for e in range(per):
            src = sd.at[pl.ds(e * ff, ff), cols] if p == 0 else wd.at[e, :, cols]
            out.append(pltpu.make_async_copy(src, w.at[slot, e, pl.ds(0, ff), :], w_sem.at[slot, len(out)]))
        return out

    def go(copies):
        for one in copies:
            one.start()

    def done(copies):
        for one in copies:
            one.wait()

    def fetch_in_up(p, q):
        @pl.when(q < n_up)
        def _():
            go(up_tile(p, q))

        @pl.when(q >= n_up)
        def _():
            go(down_tile(p, q))

    def fetch_in_down(p, q):
        @pl.when(q < n_tiles)
        def _():
            go(down_tile(p, q))

        if p + 1 < passes:
            @pl.when(q >= n_tiles)
            def _():
                go(up_tile(p + 1, q - n_tiles))

    def ups(p, lhs):
        def some(ts):
            for t in ts:
                done(up_tile(p, t))
            for t in ts:
                fetch_in_up(p, t + ahead)
            for t in ts:
                for e in range(per):
                    v = swiglu(dot(lhs(e), w[slot_of(p, t), e]))
                    h[e, :, pl.ds(pl.multiple_of(t * LANE, LANE), LANE)] = v

        @pl.loop(0, n_up // 2)
        def _(i):
            some((2 * i, 2 * i + 1))

        some((jnp.int32(n_up - 1),))

    def downs(p, store):
        @pl.loop(0, n_down // 2)
        def _(i):
            ts = (n_up + 2 * i, n_up + 2 * i + 1)
            for t in ts:
                done(down_tile(p, t))
            for t in ts:
                fetch_in_down(p, t + ahead)
            for t in ts:
                cols = pl.ds(pl.multiple_of((t - n_up) * WIDE, WIDE), WIDE)
                store(cols, *(dot(h[e], w[slot_of(p, t), e, pl.ds(0, ff), :]) for e in range(per)))

    def expert_ups(p, a, b):
        def lhs(e):
            these = pl.ds(e * last, rows)
            return jnp.concatenate([z[*a, these, :], z[*b, these, :]], axis=0)
        ups(p, lhs)

    def expert_downs(p, a, b):
        def store(cols, first, second):
            for k, ref in enumerate((a, b)):
                v, u = (o[k * rows:(k + 1) * rows] for o in (first, second))
                row = lax.broadcasted_iota(jnp.int32, (rows - last, WIDE), 0)
                edge = jnp.where(row < group - last, v[last:], u[:rows - last])
                ref[pl.ds(0, last), cols] = v[:last].astype(BF16)
                ref[pl.ds(last, rows - last), cols] = edge.astype(BF16)
                ref[pl.ds(rows, last), cols] = u[rows - last:].astype(BF16)
        downs(p, store)

    def routing():
        def place(to, here):
            away = lax.rem(to - here + side, side)
            return away ^ lax.shift_right_logical(away, 1)

        tos, spots, numbers = [], [], []
        number = lax.broadcasted_iota(jnp.int32, (1, tokens), 1).astype(F32) + 1.0
        n_to = OFFSETS * units
        for k in range(expert_ref.shape[0]):
            expert, slot = expert_ref[k], slot_ref[k]
            device, e = lax.div(expert, per), lax.rem(expert, per)
            other = lax.rem(device, 2) ^ core
            chip_to = lax.div(device, 2)
            ty, tx = lax.rem(chip_to, side), lax.div(chip_to, side)
            ta, tb = tx + (ty - tx) * core, ty + (tx - ty) * core
            oa, ob = place(ta, pa), place(tb, pb)
            u = jnp.where(ob == HERE, other, jnp.where(ob == FAR, index[FAR, SAME] + other, ob + 1 + 2 * other))
            to = u * OFFSETS + oa
            spot = jnp.where(slot < slots, (e * OFFSETS + oa) * slots + slot, -1)
            tos.append(jnp.where(lax.broadcasted_iota(jnp.int32, (n_to, tokens), 0) == to, 1.0, 0.0).astype(BF16))
            hit = lax.broadcasted_iota(jnp.int32, (full, tokens), 0) == spot
            spots.append(jnp.where(hit, number, 0.0).astype(BF16))
            numbers.append(jnp.where(hit, gate_ref[k], 0.0).astype(BF16))
        a = jnp.concatenate(tos, axis=1)
        for v, b in enumerate((spots, numbers)):
            found = lax.dot_general(a, jnp.concatenate(b, axis=1), (((1,), (1,)), ((), ())),
                                    preferred_element_type=F32)
            for u in range(units):
                for oa in range(OFFSETS):
                    k = u * OFFSETS + oa
                    mg[HERE, oa, v:v + 1, pl.ds(u * full, full)] = found[k:k + 1]

    inputs = [
        pltpu.make_async_copy(src, dst, in_sem.at[k]) for k, (src, dst) in enumerate((
            (x_hbm, xg.at[HERE]), (expert_hbm, expert_ref), (slot_hbm, slot_ref), (gate_hbm, gate_ref)))]
    with scope("enter"):
        go(inputs)
        barrier = pltpu.get_barrier_semaphore()
        peers = [at(da, db, j) for da, db in ((1, 0), (-1, 0), (0, 1), (0, -1)) for j in (SAME, OTHER)]
        peers.append(at(0, 0, OTHER))
        for peer in peers:
            pl.semaphore_signal(barrier, inc=1, device_id={"ep": peer}, device_id_type=MESH)
    with scope("x_in"):
        done(inputs)
        pl.semaphore_wait(barrier, len(peers))
        for k in range(2):
            start(("x", ON, k), ("x", BACK, k))
        for t in range(ahead):
            go(up_tile(0, t))
    with scope("routing"):
        routing()
        if full > unit:
            r[:, pl.ds(unit, full - unit), :] = jnp.zeros((units, full - unit, d), BF16)
        start(("m", ON), ("m", BACK), ("m", FAR))

    with scope("shared_up"):
        ups(0, lambda e: xg[HERE])

    def shared_store(cols, first, second):
        ysh[:, cols] = first + second

    with scope("x_wait"):
        for i in (ON, BACK):
            arrived(("x", i, 0))
            start(("xx", i))
        arrived(("m", FAR))
        start("mm")
    with scope("shared_down"):
        downs(0, shared_store)
    with scope("x_rest"):
        for i in (ON, BACK):
            arrived(("x", i, 1), ("m", i))

    def table(s, v=0):
        return mg[s, s, v:v + 1, :]

    def tables(sources):
        merged = jnp.zeros((2 * OFFSETS, total), F32)
        row = lax.broadcasted_iota(jnp.int32, merged.shape, 0)
        for s in sources:
            merged = jnp.where(row == s, table(s), merged)
        column[...] = jnp.transpose(merged)

    step = min(d, 8 * LANE)

    def gather(i, j, out, first=HERE, end=OFFSETS):
        begin = index[i, j] * full
        lane = lax.broadcasted_iota(jnp.int32, (unit, tokens), 1).astype(F32) + 1.0
        for s in range(first, end):
            token = column[pl.ds(begin, unit), s:s + 1]
            onehot[:, pl.ds(s * tokens, tokens)] = jnp.where(lane == token, 1.0, 0.0).astype(BF16)
        these = pl.ds(first * tokens, (end - first) * tokens)

        @pl.loop(0, d // step)
        def _(k):
            cols = pl.ds(pl.multiple_of(k * step, step), step)
            v = dot(onehot[:, these], xg[first:end, :, cols].reshape((end - first) * tokens, step))
            if first > HERE:
                v = v + out[:, cols].astype(F32)
            out[:, cols] = v.astype(BF16)

    early = ((FAR, SAME), (FAR, OTHER), (ON, SAME), (BACK, SAME))
    with scope("gather_early"):
        tables((HERE, ON, BACK))
        for i, j in early:
            gather(i, j, sent.at[i, j], end=FAR)
    with scope("xx_wait"):
        arrived(("xx", ON), ("xx", BACK), "mm")
    with scope("tables"):
        tables(range(OFFSETS))
    for i, j in early:
        with scope("gather_far"):
            gather(i, j, sent.at[i, j], first=FAR)
        start(("f", j) if i == FAR else ("z", i, j))
    with scope("gather"):
        gather(HERE, OTHER, sent.at[HERE, OTHER])
        start(("z", HERE, OTHER))
        gather(HERE, SAME, z.at[SAME, HERE])
        gather(ON, OTHER, sent.at[ON, OTHER])
        gather(BACK, OTHER, sent.at[BACK, OTHER])

    with scope("wait_here"):
        arrived(("z", HERE, OTHER))
    with scope("ffn_here_up"):
        expert_ups(1, (SAME, HERE), (OTHER, HERE))
    with scope("wait_f"):
        for j in (SAME, OTHER):
            arrived(("f", j))
            start(("z", FAR, j))
    start(("z", ON, OTHER), ("z", BACK, OTHER))
    with scope("ffn_here_down"):
        expert_downs(1, r.at[index[HERE, SAME]], z.at[OTHER, HERE])
    start(("r", HERE, OTHER))
    with scope("wait_same"):
        arrived(("z", ON, SAME), ("z", BACK, SAME))
    with scope("ffn_same"):
        expert_ups(2, (SAME, ON), (SAME, BACK))
        expert_downs(2, z.at[SAME, ON], z.at[SAME, BACK])
    start(("r", ON, SAME), ("r", BACK, SAME))
    with scope("wait_far"):
        arrived(("z", FAR, SAME), ("z", FAR, OTHER))
    with scope("ffn_far"):
        expert_ups(3, (SAME, FAR), (OTHER, FAR))
        expert_downs(3, z.at[SAME, FAR], z.at[OTHER, FAR])
    start(("g", SAME), ("g", OTHER))
    with scope("wait_other"):
        arrived(("z", ON, OTHER), ("z", BACK, OTHER))
    with scope("ffn_other_up"):
        expert_ups(4, (OTHER, ON), (OTHER, BACK))
    with scope("ffn_other_down"):
        expert_downs(4, z.at[OTHER, ON], z.at[OTHER, BACK])
    start(("r", ON, OTHER), ("r", BACK, OTHER))
    with scope("wait_g"):
        for j in (SAME, OTHER):
            arrived(("g", j))
            start(("r", FAR, j))
    with scope("wait_r_near"):
        arrived(*(("r", i, j) for i, j in UNITS[1:] if i != FAR))

    def weigh(s):
        token = lax.broadcasted_iota(jnp.int32, (tokens, total), 0).astype(F32) + 1.0
        combine[...] = jnp.where(token == table(s), table(s, 1), 0.0).astype(BF16)

    def add_up(store, first=0, end=units):
        these = pl.ds(first * full, (end - first) * full)

        @pl.loop(0, d // step)
        def _(k):
            cols = pl.ds(pl.multiple_of(k * step, step), step)
            store(cols, dot(combine[:, these], r[first:end, :, cols].reshape((end - first) * full, step)))

    def begin_far(cols, o):
        near[0, :, cols] = o[:half]
        near[1, :, cols] = o[half:]

    def keep_far(cols, o):
        part[2, lo, cols] = (near[0, :, cols] + o[:half]).astype(BF16)
        part[2, hi, cols] = (near[1, :, cols] + o[half:]).astype(BF16)

    def keep_next(cols, o):
        near[0, :, cols] = o[:half]
        part[0, hi, cols] = o[half:].astype(BF16)

    def keep_back(cols, o):
        near[1, :, cols] = o[half:]
        part[1, lo, cols] = o[:half].astype(BF16)

    def keep_own(cols, o):
        ysh[:, cols] = ysh[:, cols] + o

    with scope("sum_far_early"):
        weigh(FAR)
        add_up(begin_far, end=index[FAR, SAME])
    with scope("wait_r_far"):
        arrived(("r", FAR, SAME), ("r", FAR, OTHER))
    with scope("sum_far"):
        add_up(keep_far, first=index[FAR, SAME])
    start(("pp", 0), ("pp", 1))
    with scope("sum_near"):
        weigh(BACK)
        add_up(keep_next)
        start(("p", 0, 0))
        weigh(ON)
        add_up(keep_back)
        start(("p", 1, 0))
    with scope("wait_pp"):
        for k, first in ((0, lo), (1, hi)):
            arrived(("pp", k))
            part[k, first, :] = (near[k] + rfar[k].astype(F32)).astype(BF16)
            start(("p", k, 1))
    with scope("sum_own"):
        weigh(HERE)
        add_up(keep_own)
    with scope("wait_p"):
        arrived(*(("p", k, v) for k in range(2) for v in range(2)))
    with scope("leave"):
        y_ref[...] = (ysh[...] + (rn[0].astype(F32) + rn[1].astype(F32))).astype(y_ref.dtype)
        for one in c.values():
            one.wait_send()


def solution(mesh):
    side = math.isqrt(mesh.shape["ep"] // 2)
    assert side == OFFSETS

    def local(x, expert, slot, gate, w_gate, w_up, w_down, s_gate, s_up, s_down):
        tokens, d = x.shape[2:]
        top = expert.shape[3]
        per, _, ff = w_gate.shape
        experts = per * mesh.shape["ep"]
        slots = 5 * tokens * top // (4 * experts)
        unit = per * OFFSETS * slots
        full = unit + (-unit) % LANE
        half, units = tokens // 2, len(UNITS)
        choices = (v.transpose(0, 3, 1, 2).reshape(top, 1, tokens) for v in (expert, slot, gate))
        anywhere, vmem = pl.BlockSpec(memory_space=pl.ANY), pl.BlockSpec(memory_space=pltpu.VMEM)
        y = pl.pallas_call(
            functools.partial(kernel, side, slots),
            out_shape=jax.ShapeDtypeStruct((tokens, d), x.dtype),
            in_specs=[anywhere] * 10,
            out_specs=vmem,
            scratch_shapes=[
                *(pltpu.VMEM((top, 1, tokens), v.dtype) for v in (expert, slot, gate)),
                pltpu.VMEM((OFFSETS, tokens, d), BF16),
                pltpu.VMEM((OFFSETS, OFFSETS, 2, units * full), F32),
                pltpu.VMEM((units * full, 2 * OFFSETS), F32),
                pltpu.VMEM((unit, OFFSETS * tokens), BF16),
                pltpu.VMEM((tokens, units * full), BF16),
                pltpu.VMEM((OFFSETS, 2, unit, d), BF16),
                pltpu.VMEM((2, unit, d), BF16),
                pltpu.VMEM((2, OFFSETS, unit, d), BF16),
                pltpu.VMEM((units, full, d), BF16),
                pltpu.VMEM((2, unit, d), BF16),
                pltpu.VMEM((per, 2 * (unit // per + 8), ff), BF16),
                pltpu.VMEM((BUFFERS, per, d, WIDE), BF16),
                pltpu.VMEM((3, tokens, d), BF16),
                pltpu.VMEM((2, half, d), F32),
                pltpu.VMEM((2, half, d), BF16),
                pltpu.VMEM((2, tokens, d), BF16),
                pltpu.VMEM((tokens, d), F32),
                pltpu.SemaphoreType.DMA((4,)),
                pltpu.SemaphoreType.DMA((BUFFERS, 4)),
                pltpu.SemaphoreType.DMA((COPIES,)),
                pltpu.SemaphoreType.DMA((COPIES,)),
            ],
            compiler_params=pltpu.CompilerParams(
                collective_id=0, has_side_effects=True, vmem_limit_bytes=67_000_000),
            name="moe",
        )(x.reshape(tokens, d), *choices, w_gate, w_up, w_down, s_gate, s_up, s_down)
        return y.reshape(x.shape)

    spread, held, whole = P("dp", "ep", None, None), P("ep", None, None), P(None, None)
    return jax.shard_map(
        local, mesh=mesh, in_specs=(spread,) * 4 + (held,) * 3 + (whole,) * 3, out_specs=spread, check_vma=False)
```

```python
import contextlib
import functools
import math

import jax
import jax.numpy as jnp
from jax import lax
from jax.experimental import pallas as pl
from jax.experimental.pallas import tpu as pltpu
from jax.sharding import PartitionSpec as P

MESH = pl.DeviceIdType.MESH
OFFSETS = 4
HERE, ON, BACK, FAR = range(OFFSETS)
SAME, OTHER = range(2)
UNITS = ((HERE, SAME), (HERE, OTHER), (ON, SAME), (BACK, SAME), (ON, OTHER), (BACK, OTHER), (FAR, SAME), (FAR, OTHER))
LANE = 128
WIDE = 2 * LANE
BUFFERS = 6
COPIES = 34
BF16, F32 = jnp.bfloat16, jnp.float32
scope = contextlib.nullcontext


def dot(a, b):
    return jnp.dot(a, b, preferred_element_type=F32)


def swiglu(both):
    g, u = both[:, :LANE], both[:, LANE:]
    return (g * jax.nn.sigmoid(g) * u).astype(BF16)


def kernel(side, slots, x_hbm, expert_hbm, slot_hbm, gate_hbm, wg, wu, wd, sg, su, sd, y_ref,
           expert_ref, slot_ref, gate_ref, xg, mg, column, onehot, combine, sent, fwd, z, r, fwdb, h, w, part, near, rfar, rn, ysh,
           in_sem, w_sem, send_sem, recv_sem):
    tokens, d = x_hbm.shape
    per, _, ff = wg.shape
    group = OFFSETS * slots
    unit = per * group
    rows = group + (-group) % 16
    last = unit - rows
    half = tokens // 2
    full = unit + (-unit) % LANE
    units = len(UNITS)
    total = units * full
    index = {u: k for k, u in enumerate(UNITS)}

    me = lax.axis_index("ep")
    core, chip = lax.rem(me, 2), lax.div(me, 2)
    py, px = lax.rem(chip, side), lax.div(chip, side)
    pa, pb = px + (py - px) * core, py + (px - py) * core
    sa, sb = 2 * side - (2 * side - 2) * core, 2 + (2 * side - 2) * core

    def at(da, db, other):
        a, b = lax.rem(pa + da + side, side), lax.rem(pb + db + side, side)
        return sa * a + sb * b + (1 - core if other else core)

    def copy(i, src, dst, to):
        return pltpu.make_async_remote_copy(
            src_ref=src, dst_ref=dst, send_sem=send_sem.at[i], recv_sem=recv_sem.at[i],
            device_id={"ep": to}, device_id_type=MESH)

    lo, hi, body = pl.ds(0, half), pl.ds(half, half), pl.ds(0, unit)
    c = {}

    def link(name, src, dst, to):
        c[name] = copy(len(c), src, dst, to)

    def back(i, j):
        return r.at[index[i, j], body]

    for i, way, first, second in ((ON, 1, lo, hi), (BACK, -1, hi, lo)):
        link(("x", i, 0), xg.at[HERE, first], xg.at[i, first], at(way, 0, SAME))
        link(("x", i, 1), xg.at[HERE, second], xg.at[i, second], at(way, 0, SAME))
        link(("m", i), mg.at[HERE, i], mg.at[i, i], at(way, 0, SAME))
        link(("xx", i), xg.at[i, first], xg.at[FAR, first], at(way, 0, SAME))
    link(("m", FAR), mg.at[HERE, FAR], mg.at[ON, FAR], at(1, 0, SAME))
    link("mm", mg.at[ON, FAR], mg.at[FAR, FAR], at(1, 0, SAME))
    link(("z", HERE, OTHER), sent.at[HERE, OTHER], z.at[OTHER, HERE], at(0, 0, OTHER))
    link(("r", HERE, OTHER), z.at[OTHER, HERE], back(HERE, OTHER), at(0, 0, OTHER))
    for i, way in ((ON, 1), (BACK, -1)):
        for j in (SAME, OTHER):
            link(("z", i, j), sent.at[i, j], z.at[j, i], at(0, way, j))
        link(("r", i, SAME), z.at[SAME, i], back(i, SAME), at(0, -way, SAME))
        link(("r", i, OTHER), z.at[OTHER, i], back(i, OTHER), at(-way, 0, OTHER))
    for j, way in ((SAME, 1), (OTHER, -1)):
        link(("f", j), sent.at[FAR, j], fwd.at[j], at(0, way, SAME))
        link(("z", FAR, j), fwd.at[j], z.at[j, FAR], at(0, way, j))
        link(("r", FAR, j), fwdb.at[j], back(FAR, j), at(0, -way, SAME))
    link(("g", SAME), z.at[SAME, FAR], fwdb.at[SAME], at(0, -1, SAME))
    link(("g", OTHER), z.at[OTHER, FAR], fwdb.at[OTHER], at(1, 0, OTHER))
    for k, way, first, second in ((0, 1, lo, hi), (1, -1, hi, lo)):
        link(("pp", k), part.at[2, first], rfar.at[k], at(way, 0, SAME))
        link(("p", k, 0), part.at[k, second], rn.at[k, second], at(way, 0, SAME))
        link(("p", k, 1), part.at[k, first], rn.at[k, first], at(way, 0, SAME))
    assert len(c) == COPIES

    def start(*which):
        for i in which:
            c[i].start()

    def arrived(*which):
        for i in which:
            c[i].wait_recv()

    n_up, n_down, passes = ff // LANE, d // WIDE, 5
    n_tiles = n_up + n_down
    ahead = BUFFERS - 2
    assert per == 2 and n_up % 2 == 1 and n_down % 2 == 0

    def slot_of(p, t):
        return lax.rem(p * n_tiles + t, BUFFERS)

    def up_tile(p, t):
        slot = slot_of(p, t)
        out = []
        for e in range(per):
            for k, (shared, own) in enumerate(((sg, wg), (su, wu))):
                if p == 0:
                    src = shared.at[:, pl.ds(pl.multiple_of(e * ff + t * LANE, LANE), LANE)]
                else:
                    src = own.at[e, :, pl.ds(pl.multiple_of(t * LANE, LANE), LANE)]
                out.append(pltpu.make_async_copy(
                    src, w.at[slot, e, :, pl.ds(k * LANE, LANE)], w_sem.at[slot, len(out)]))
        return out

    def down_tile(p, t):
        slot = slot_of(p, t)
        cols = pl.ds(pl.multiple_of((t - n_up) * WIDE, WIDE), WIDE)
        out = []
        for e in range(per):
            src = sd.at[pl.ds(e * ff, ff), cols] if p == 0 else wd.at[e, :, cols]
            out.append(pltpu.make_async_copy(src, w.at[slot, e, pl.ds(0, ff), :], w_sem.at[slot, len(out)]))
        return out

    def go(copies):
        for one in copies:
            one.start()

    def done(copies):
        for one in copies:
            one.wait()

    def fetch_in_up(p, q):
        @pl.when(q < n_up)
        def _():
            go(up_tile(p, q))

        @pl.when(q >= n_up)
        def _():
            go(down_tile(p, q))

    def fetch_in_down(p, q):
        @pl.when(q < n_tiles)
        def _():
            go(down_tile(p, q))

        if p + 1 < passes:
            @pl.when(q >= n_tiles)
            def _():
                go(up_tile(p + 1, q - n_tiles))

    def ups(p, lhs):
        def some(ts):
            for t in ts:
                done(up_tile(p, t))
            for t in ts:
                fetch_in_up(p, t + ahead)
            for t in ts:
                for e in range(per):
                    v = swiglu(dot(lhs(e), w[slot_of(p, t), e]))
                    h[e, :, pl.ds(pl.multiple_of(t * LANE, LANE), LANE)] = v

        @pl.loop(0, n_up // 2)
        def _(i):
            some((2 * i, 2 * i + 1))

        some((jnp.int32(n_up - 1),))

    def downs(p, store):
        @pl.loop(0, n_down // 2)
        def _(i):
            ts = (n_up + 2 * i, n_up + 2 * i + 1)
            for t in ts:
                done(down_tile(p, t))
            for t in ts:
                fetch_in_down(p, t + ahead)
            for t in ts:
                cols = pl.ds(pl.multiple_of((t - n_up) * WIDE, WIDE), WIDE)
                store(cols, *(dot(h[e], w[slot_of(p, t), e, pl.ds(0, ff), :]) for e in range(per)))

    def expert_ups(p, a, b):
        def lhs(e):
            these = pl.ds(e * last, rows)
            return jnp.concatenate([z[*a, these, :], z[*b, these, :]], axis=0)
        ups(p, lhs)

    def expert_downs(p, a, b):
        def store(cols, first, second):
            for k, ref in enumerate((a, b)):
                v, u = (o[k * rows:(k + 1) * rows] for o in (first, second))
                row = lax.broadcasted_iota(jnp.int32, (rows - last, WIDE), 0)
                edge = jnp.where(row < group - last, v[last:], u[:rows - last])
                ref[pl.ds(0, last), cols] = v[:last].astype(BF16)
                ref[pl.ds(last, rows - last), cols] = edge.astype(BF16)
                ref[pl.ds(rows, last), cols] = u[rows - last:].astype(BF16)
        downs(p, store)

    def routing():
        def place(to, here):
            away = lax.rem(to - here + side, side)
            return away ^ lax.shift_right_logical(away, 1)

        tos, spots, numbers = [], [], []
        number = lax.broadcasted_iota(jnp.int32, (1, tokens), 1).astype(F32) + 1.0
        n_to = OFFSETS * units
        for k in range(expert_ref.shape[0]):
            expert, slot = expert_ref[k], slot_ref[k]
            device, e = lax.div(expert, per), lax.rem(expert, per)
            other = lax.rem(device, 2) ^ core
            chip_to = lax.div(device, 2)
            ty, tx = lax.rem(chip_to, side), lax.div(chip_to, side)
            ta, tb = tx + (ty - tx) * core, ty + (tx - ty) * core
            oa, ob = place(ta, pa), place(tb, pb)
            u = jnp.where(ob == HERE, other, jnp.where(ob == FAR, index[FAR, SAME] + other, ob + 1 + 2 * other))
            to = u * OFFSETS + oa
            spot = jnp.where(slot < slots, (e * OFFSETS + oa) * slots + slot, -1)
            tos.append(jnp.where(lax.broadcasted_iota(jnp.int32, (n_to, tokens), 0) == to, 1.0, 0.0).astype(BF16))
            hit = lax.broadcasted_iota(jnp.int32, (full, tokens), 0) == spot
            spots.append(jnp.where(hit, number, 0.0).astype(BF16))
            numbers.append(jnp.where(hit, gate_ref[k], 0.0).astype(BF16))
        a = jnp.concatenate(tos, axis=1)
        for v, b in enumerate((spots, numbers)):
            found = lax.dot_general(a, jnp.concatenate(b, axis=1), (((1,), (1,)), ((), ())),
                                    preferred_element_type=F32)
            for u in range(units):
                for oa in range(OFFSETS):
                    k = u * OFFSETS + oa
                    mg[HERE, oa, v:v + 1, pl.ds(u * full, full)] = found[k:k + 1]

    inputs = [
        pltpu.make_async_copy(src, dst, in_sem.at[k]) for k, (src, dst) in enumerate((
            (x_hbm, xg.at[HERE]), (expert_hbm, expert_ref), (slot_hbm, slot_ref), (gate_hbm, gate_ref)))]
    with scope("enter"):
        go(inputs)
        barrier = pltpu.get_barrier_semaphore()
        peers = [at(da, db, j) for da, db in ((1, 0), (-1, 0), (0, 1), (0, -1)) for j in (SAME, OTHER)]
        peers.append(at(0, 0, OTHER))
        for peer in peers:
            pl.semaphore_signal(barrier, inc=1, device_id={"ep": peer}, device_id_type=MESH)
    with scope("x_in"):
        done(inputs)
        for t in range(ahead):
            go(up_tile(0, t))
        pl.semaphore_wait(barrier, len(peers))
        start(("x", ON, 0), ("x", BACK, 0))
    with scope("routing"):
        routing()
        if full > unit:
            r[:, pl.ds(unit, full - unit), :] = jnp.zeros((units, full - unit, d), BF16)
        start(("m", FAR), ("x", ON, 1), ("x", BACK, 1), ("m", ON), ("m", BACK))

    with scope("shared_up"):
        ups(0, lambda e: xg[HERE])

    def shared_store(cols, first, second):
        ysh[:, cols] = first + second

    with scope("x_wait"):
        for i in (ON, BACK):
            arrived(("x", i, 0))
            start(("xx", i))
    with scope("shared_down"):
        downs(0, shared_store)
    with scope("wait_mm"):
        arrived(("m", FAR))
        start("mm")
    with scope("x_rest"):
        for i in (ON, BACK):
            arrived(("x", i, 1), ("m", i))

    def table(s, v=0):
        return mg[s, s, v:v + 1, :]

    def tables(sources):
        merged = jnp.zeros((2 * OFFSETS, total), F32)
        row = lax.broadcasted_iota(jnp.int32, merged.shape, 0)
        for s in sources:
            merged = jnp.where(row == s, table(s), merged)
        column[...] = jnp.transpose(merged)

    step = min(d, 8 * LANE)

    def gather(i, j, out, first=HERE, end=OFFSETS):
        begin = index[i, j] * full
        lane = lax.broadcasted_iota(jnp.int32, (unit, tokens), 1).astype(F32) + 1.0
        for s in range(first, end):
            token = column[pl.ds(begin, unit), s:s + 1]
            onehot[:, pl.ds(s * tokens, tokens)] = jnp.where(lane == token, 1.0, 0.0).astype(BF16)
        these = pl.ds(first * tokens, (end - first) * tokens)

        @pl.loop(0, d // step)
        def _(k):
            cols = pl.ds(pl.multiple_of(k * step, step), step)
            v = dot(onehot[:, these], xg[first:end, :, cols].reshape((end - first) * tokens, step))
            if first > HERE:
                v = v + out[:, cols].astype(F32)
            out[:, cols] = v.astype(BF16)

    early = ((FAR, SAME), (FAR, OTHER), (ON, SAME), (BACK, SAME))
    with scope("gather_early"):
        tables((HERE, ON, BACK))
        for i, j in early:
            gather(i, j, sent.at[i, j], end=FAR)
    with scope("xx_wait"):
        arrived(("xx", ON), ("xx", BACK), "mm")
    with scope("tables"):
        tables(range(OFFSETS))
    for i, j in early:
        with scope("gather_far"):
            gather(i, j, sent.at[i, j], first=FAR)
        start(("f", j) if i == FAR else ("z", i, j))
    with scope("gather"):
        gather(HERE, OTHER, sent.at[HERE, OTHER])
        start(("z", HERE, OTHER))
        gather(HERE, SAME, z.at[SAME, HERE])
        gather(ON, OTHER, sent.at[ON, OTHER])
        gather(BACK, OTHER, sent.at[BACK, OTHER])

    with scope("wait_here"):
        arrived(("z", HERE, OTHER))
    with scope("ffn_here_up"):
        expert_ups(1, (SAME, HERE), (OTHER, HERE))
    with scope("wait_f"):
        for j in (SAME, OTHER):
            arrived(("f", j))
            start(("z", FAR, j))
    start(("z", ON, OTHER), ("z", BACK, OTHER))
    with scope("ffn_here_down"):
        expert_downs(1, r.at[index[HERE, SAME]], z.at[OTHER, HERE])
    start(("r", HERE, OTHER))
    with scope("wait_same"):
        arrived(("z", ON, SAME), ("z", BACK, SAME))
    with scope("ffn_same"):
        expert_ups(2, (SAME, ON), (SAME, BACK))
        expert_downs(2, z.at[SAME, ON], z.at[SAME, BACK])
    start(("r", ON, SAME), ("r", BACK, SAME))
    with scope("wait_far"):
        arrived(("z", FAR, SAME), ("z", FAR, OTHER))
    with scope("ffn_far"):
        expert_ups(3, (SAME, FAR), (OTHER, FAR))
        expert_downs(3, z.at[SAME, FAR], z.at[OTHER, FAR])
    start(("g", SAME), ("g", OTHER))
    with scope("wait_other"):
        arrived(("z", ON, OTHER), ("z", BACK, OTHER))
    with scope("ffn_other_up"):
        expert_ups(4, (OTHER, ON), (OTHER, BACK))
    with scope("ffn_other_down"):
        expert_downs(4, z.at[OTHER, ON], z.at[OTHER, BACK])
    start(("r", ON, OTHER), ("r", BACK, OTHER))
    with scope("wait_g"):
        for j in (SAME, OTHER):
            arrived(("g", j))
            start(("r", FAR, j))
    with scope("wait_r_near"):
        arrived(*(("r", i, j) for i, j in UNITS[1:] if i != FAR))

    def weigh(s):
        token = lax.broadcasted_iota(jnp.int32, (tokens, total), 0).astype(F32) + 1.0
        combine[...] = jnp.where(token == table(s), table(s, 1), 0.0).astype(BF16)

    def add_up(store, first=0, end=units):
        these = pl.ds(first * full, (end - first) * full)

        @pl.loop(0, d // step)
        def _(k):
            cols = pl.ds(pl.multiple_of(k * step, step), step)
            store(cols, dot(combine[:, these], r[first:end, :, cols].reshape((end - first) * full, step)))

    def begin_far(cols, o):
        near[0, :, cols] = o[:half]
        near[1, :, cols] = o[half:]

    def keep_far(cols, o):
        part[2, lo, cols] = (near[0, :, cols] + o[:half]).astype(BF16)
        part[2, hi, cols] = (near[1, :, cols] + o[half:]).astype(BF16)

    def keep_next(cols, o):
        near[0, :, cols] = o[:half]
        part[0, hi, cols] = o[half:].astype(BF16)

    def keep_back(cols, o):
        near[1, :, cols] = o[half:]
        part[1, lo, cols] = o[:half].astype(BF16)

    def keep_own(cols, o):
        ysh[:, cols] = ysh[:, cols] + o

    with scope("sum_far_early"):
        weigh(FAR)
        add_up(begin_far, end=index[FAR, SAME])
    with scope("wait_r_far"):
        arrived(("r", FAR, SAME), ("r", FAR, OTHER))
    with scope("sum_far"):
        add_up(keep_far, first=index[FAR, SAME])
    start(("pp", 0), ("pp", 1))
    with scope("sum_near"):
        weigh(BACK)
        add_up(keep_next)
        start(("p", 0, 0))
        weigh(ON)
        add_up(keep_back)
        start(("p", 1, 0))
    with scope("wait_pp"):
        for k, first in ((0, lo), (1, hi)):
            arrived(("pp", k))
            part[k, first, :] = (near[k] + rfar[k].astype(F32)).astype(BF16)
            start(("p", k, 1))
    with scope("sum_own"):
        weigh(HERE)
        add_up(keep_own)
    with scope("wait_p"):
        arrived(*(("p", k, v) for k in range(2) for v in range(2)))
    with scope("leave"):
        y_ref[...] = (ysh[...] + (rn[0].astype(F32) + rn[1].astype(F32))).astype(y_ref.dtype)
        for one in c.values():
            one.wait_send()


def solution(mesh):
    side = math.isqrt(mesh.shape["ep"] // 2)
    assert side == OFFSETS

    def local(x, expert, slot, gate, w_gate, w_up, w_down, s_gate, s_up, s_down):
        tokens, d = x.shape[2:]
        top = expert.shape[3]
        per, _, ff = w_gate.shape
        experts = per * mesh.shape["ep"]
        slots = 5 * tokens * top // (4 * experts)
        unit = per * OFFSETS * slots
        full = unit + (-unit) % LANE
        half, units = tokens // 2, len(UNITS)
        choices = (v.transpose(0, 3, 1, 2).reshape(top, 1, tokens) for v in (expert, slot, gate))
        anywhere, vmem = pl.BlockSpec(memory_space=pl.ANY), pl.BlockSpec(memory_space=pltpu.VMEM)
        y = pl.pallas_call(
            functools.partial(kernel, side, slots),
            out_shape=jax.ShapeDtypeStruct((tokens, d), x.dtype),
            in_specs=[anywhere] * 10,
            out_specs=vmem,
            scratch_shapes=[
                *(pltpu.VMEM((top, 1, tokens), v.dtype) for v in (expert, slot, gate)),
                pltpu.VMEM((OFFSETS, tokens, d), BF16),
                pltpu.VMEM((OFFSETS, OFFSETS, 2, units * full), F32),
                pltpu.VMEM((units * full, 2 * OFFSETS), F32),
                pltpu.VMEM((unit, OFFSETS * tokens), BF16),
                pltpu.VMEM((tokens, units * full), BF16),
                pltpu.VMEM((OFFSETS, 2, unit, d), BF16),
                pltpu.VMEM((2, unit, d), BF16),
                pltpu.VMEM((2, OFFSETS, unit, d), BF16),
                pltpu.VMEM((units, full, d), BF16),
                pltpu.VMEM((2, unit, d), BF16),
                pltpu.VMEM((per, 2 * (unit // per + 8), ff), BF16),
                pltpu.VMEM((BUFFERS, per, d, WIDE), BF16),
                pltpu.VMEM((3, tokens, d), BF16),
                pltpu.VMEM((2, half, d), F32),
                pltpu.VMEM((2, half, d), BF16),
                pltpu.VMEM((2, tokens, d), BF16),
                pltpu.VMEM((tokens, d), F32),
                pltpu.SemaphoreType.DMA((4,)),
                pltpu.SemaphoreType.DMA((BUFFERS, 4)),
                pltpu.SemaphoreType.DMA((COPIES,)),
                pltpu.SemaphoreType.DMA((COPIES,)),
            ],
            compiler_params=pltpu.CompilerParams(
                collective_id=0, has_side_effects=True, vmem_limit_bytes=67_000_000),
            name="moe",
        )(x.reshape(tokens, d), *choices, w_gate, w_up, w_down, s_gate, s_up, s_down)
        return y.reshape(x.shape)

    spread, held, whole = P("dp", "ep", None, None), P("ep", None, None), P(None, None)
    return jax.shard_map(
        local, mesh=mesh, in_specs=(spread,) * 4 + (held,) * 3 + (whole,) * 3, out_specs=spread, check_vma=False)
```

```python
import contextlib
import functools
import math

import jax
import jax.numpy as jnp
from jax import lax
from jax.experimental import pallas as pl
from jax.experimental.pallas import tpu as pltpu
from jax.sharding import PartitionSpec as P

MESH = pl.DeviceIdType.MESH
OFFSETS = 4
HERE, ON, BACK, FAR = range(OFFSETS)
SAME, OTHER = range(2)
UNITS = ((HERE, SAME), (HERE, OTHER), (ON, SAME), (BACK, SAME), (ON, OTHER), (BACK, OTHER), (FAR, SAME), (FAR, OTHER))
LANE = 128
WIDE = 2 * LANE
BUFFERS = 6
COPIES = 58
BF16, F32 = jnp.bfloat16, jnp.float32
scope = contextlib.nullcontext


def dot(a, b):
    return jnp.dot(a, b, preferred_element_type=F32)


def swiglu(both):
    g, u = both[:, :LANE], both[:, LANE:]
    return (g * jax.nn.sigmoid(g) * u).astype(BF16)


def kernel(side, slots, x_hbm, expert_hbm, slot_hbm, gate_hbm, wg, wu, wd, sg, su, sd, y_hbm,
           expert_ref, slot_ref, gate_ref, xg, mg, column, onehot, ybuf, sent, fwd, z, r, fwdb, h, w, part, near, rfar, rn, ysh,
           in_sem, w_sem, send_sem, recv_sem):
    tokens, d = x_hbm.shape
    per, _, ff = wg.shape
    group = OFFSETS * slots
    unit = per * group
    rows = group + (-group) % 16
    last = unit - rows
    half = tokens // 2
    full = unit + (-unit) % LANE
    units = len(UNITS)
    total = units * full
    index = {u: k for k, u in enumerate(UNITS)}

    me = lax.axis_index("ep")
    core, chip = lax.rem(me, 2), lax.div(me, 2)
    py, px = lax.rem(chip, side), lax.div(chip, side)
    pa, pb = px + (py - px) * core, py + (px - py) * core
    sa, sb = 2 * side - (2 * side - 2) * core, 2 + (2 * side - 2) * core

    def at(da, db, other):
        a, b = lax.rem(pa + da + side, side), lax.rem(pb + db + side, side)
        return sa * a + sb * b + (1 - core if other else core)

    def copy(i, src, dst, to):
        return pltpu.make_async_remote_copy(
            src_ref=src, dst_ref=dst, send_sem=send_sem.at[i], recv_sem=recv_sem.at[i],
            device_id={"ep": to}, device_id_type=MESH)

    lo, hi, body = pl.ds(0, half), pl.ds(half, half), pl.ds(0, unit)
    sides = pl.ds(0, d // 2), pl.ds(d // 2, d // 2)
    spans = [(e * group + (-e * group) % 16, (e * group + FAR * slots) // 16 * 16) for e in range(per)]
    free = len(spans)
    spans += [(spans[e][1], spans[e + 1][0] if e + 1 < per else unit) for e in range(per)]
    assert spans[0][0] == 0
    early = ((FAR, SAME), (FAR, OTHER), (ON, SAME), (BACK, SAME))
    c = {}

    def link(name, src, dst, to):
        c[name] = copy(len(c), src, dst, to)

    def back(i, j):
        return r.at[index[i, j], body]

    for i, way, first, second in ((ON, 1, lo, hi), (BACK, -1, hi, lo)):
        link(("x", i, 0), xg.at[HERE, first], xg.at[i, first], at(way, 0, SAME))
        link(("x", i, 1), xg.at[HERE, second], xg.at[i, second], at(way, 0, SAME))
        link(("m", i), mg.at[HERE, i], mg.at[i, i], at(way, 0, SAME))
        link(("xx", i), xg.at[i, first], xg.at[FAR, first], at(way, 0, SAME))
    link(("m", FAR), mg.at[HERE, FAR], mg.at[ON, FAR], at(1, 0, SAME))
    link("mm", mg.at[ON, FAR], mg.at[FAR, FAR], at(1, 0, SAME))
    def unit_links(i, j, dst, to):
        if (i, j) in early:
            for k, (first, end) in enumerate(spans):
                these = pl.ds(first, end - first)
                link(("s", i, j, k), sent.at[i, j, these], dst.at[these], to)
        else:
            link(("s", i, j), sent.at[i, j], dst, to)

    unit_links(HERE, OTHER, z.at[OTHER, HERE], at(0, 0, OTHER))
    link(("r", HERE, OTHER), z.at[OTHER, HERE], back(HERE, OTHER), at(0, 0, OTHER))
    for i, way in ((ON, 1), (BACK, -1)):
        for j in (SAME, OTHER):
            unit_links(i, j, z.at[j, i], at(0, way, j))
        link(("r", i, SAME), z.at[SAME, i], back(i, SAME), at(0, -way, SAME))
        for v, cols in enumerate(sides):
            link(("r", i, OTHER, v), z.at[OTHER, i, :, cols], back(i, OTHER).at[:, cols], at(-way, 0, OTHER))
    for j, way in ((SAME, 1), (OTHER, -1)):
        unit_links(FAR, j, fwd.at[j], at(0, way, SAME))
        link(("z", FAR, j), fwd.at[j], z.at[j, FAR], at(0, way, j))
        for v, cols in enumerate(sides):
            to = at(0, -1, SAME) if j == SAME else at(1, 0, OTHER)
            link(("g", j, v), z.at[j, FAR, :, cols], fwdb.at[j, :, cols], to)
            link(("r", FAR, j, v), fwdb.at[j, :, cols], back(FAR, j).at[:, cols], at(0, -way, SAME))
    for k, way, first, second in ((0, 1, lo, hi), (1, -1, hi, lo)):
        for v, cols in enumerate(sides):
            link(("pp", k, v), part.at[2, first, cols], rfar.at[k, :, cols], at(way, 0, SAME))
            link(("p", k, 0, v), part.at[k, second, cols], rn.at[k, second, cols], at(way, 0, SAME))
            link(("p", k, 1, v), part.at[k, first, cols], rn.at[k, first, cols], at(way, 0, SAME))
    assert len(c) == COPIES

    def start(*which):
        for i in which:
            c[i].start()

    def arrived(*which):
        for i in which:
            c[i].wait_recv()

    n_up, n_down, passes = ff // LANE, d // WIDE, 5
    n_tiles = n_up + n_down
    ahead = BUFFERS - 2
    assert per == 2 and n_up % 2 == 1 and n_down % 2 == 0

    def slot_of(p, t):
        return lax.rem(p * n_tiles + t, BUFFERS)

    def up_tile(p, t):
        slot = slot_of(p, t)
        out = []
        for e in range(per):
            for k, (shared, own) in enumerate(((sg, wg), (su, wu))):
                if p == 0:
                    src = shared.at[:, pl.ds(pl.multiple_of(e * ff + t * LANE, LANE), LANE)]
                else:
                    src = own.at[e, :, pl.ds(pl.multiple_of(t * LANE, LANE), LANE)]
                out.append(pltpu.make_async_copy(
                    src, w.at[slot, e, :, pl.ds(k * LANE, LANE)], w_sem.at[slot, len(out)]))
        return out

    def down_tile(p, t):
        slot = slot_of(p, t)
        cols = pl.ds(pl.multiple_of((t - n_up) * WIDE, WIDE), WIDE)
        out = []
        for e in range(per):
            src = sd.at[pl.ds(e * ff, ff), cols] if p == 0 else wd.at[e, :, cols]
            out.append(pltpu.make_async_copy(src, w.at[slot, e, pl.ds(0, ff), :], w_sem.at[slot, len(out)]))
        return out

    def go(copies):
        for one in copies:
            one.start()

    def done(copies):
        for one in copies:
            one.wait()

    def fetch_in_up(p, q):
        @pl.when(q < n_up)
        def _():
            go(up_tile(p, q))

        @pl.when(q >= n_up)
        def _():
            go(down_tile(p, q))

    def fetch_in_down(p, q):
        @pl.when(q < n_tiles)
        def _():
            go(down_tile(p, q))

        if p + 1 < passes:
            @pl.when(q >= n_tiles)
            def _():
                go(up_tile(p + 1, q - n_tiles))

    def ups(p, lhs):
        def some(ts):
            for t in ts:
                done(up_tile(p, t))
            for t in ts:
                fetch_in_up(p, t + ahead)
            for t in ts:
                for e in range(per):
                    v = swiglu(dot(lhs(e), w[slot_of(p, t), e]))
                    h[e, :, pl.ds(pl.multiple_of(t * LANE, LANE), LANE)] = v

        @pl.loop(0, n_up // 2)
        def _(i):
            some((2 * i, 2 * i + 1))

        some((jnp.int32(n_up - 1),))

    def downs(p, store, begin=0, end=n_down // 2):
        @pl.loop(begin, end)
        def _(i):
            ts = (n_up + 2 * i, n_up + 2 * i + 1)
            for t in ts:
                done(down_tile(p, t))
            for t in ts:
                fetch_in_down(p, t + ahead)
            for t in ts:
                cols = pl.ds(pl.multiple_of((t - n_up) * WIDE, WIDE), WIDE)
                store(cols, *(dot(h[e], w[slot_of(p, t), e, pl.ds(0, ff), :]) for e in range(per)))

    def expert_ups(p, a, b):
        def lhs(e):
            these = pl.ds(e * last, rows)
            return jnp.concatenate([z[*a, these, :], z[*b, these, :]], axis=0)
        ups(p, lhs)

    def expert_downs(p, a, b, *which):
        def store(cols, first, second):
            for k, ref in enumerate((a, b)):
                v, u = (o[k * rows:(k + 1) * rows] for o in (first, second))
                row = lax.broadcasted_iota(jnp.int32, (rows - last, WIDE), 0)
                edge = jnp.where(row < group - last, v[last:], u[:rows - last])
                ref[pl.ds(0, last), cols] = v[:last].astype(BF16)
                ref[pl.ds(last, rows - last), cols] = edge.astype(BF16)
                ref[pl.ds(rows, last), cols] = u[rows - last:].astype(BF16)
        downs(p, store, *which)

    def routing():
        def place(to, here):
            away = lax.rem(to - here + side, side)
            return away ^ lax.shift_right_logical(away, 1)

        tos, spots, numbers = [], [], []
        number = lax.broadcasted_iota(jnp.int32, (1, tokens), 1).astype(F32) + 1.0
        n_to = OFFSETS * units
        for k in range(expert_ref.shape[0]):
            expert, slot = expert_ref[k], slot_ref[k]
            device, e = lax.div(expert, per), lax.rem(expert, per)
            other = lax.rem(device, 2) ^ core
            chip_to = lax.div(device, 2)
            ty, tx = lax.rem(chip_to, side), lax.div(chip_to, side)
            ta, tb = tx + (ty - tx) * core, ty + (tx - ty) * core
            oa, ob = place(ta, pa), place(tb, pb)
            u = jnp.where(ob == HERE, other, jnp.where(ob == FAR, index[FAR, SAME] + other, ob + 1 + 2 * other))
            to = u * OFFSETS + oa
            spot = jnp.where(slot < slots, (e * OFFSETS + oa) * slots + slot, -1)
            tos.append(jnp.where(lax.broadcasted_iota(jnp.int32, (n_to, tokens), 0) == to, 1.0, 0.0).astype(BF16))
            hit = lax.broadcasted_iota(jnp.int32, (full, tokens), 0) == spot
            spots.append(jnp.where(hit, number, 0.0).astype(BF16))
            numbers.append(jnp.where(hit, gate_ref[k], 0.0).astype(BF16))
        a = jnp.concatenate(tos, axis=1)
        for v, b in enumerate((spots, numbers)):
            found = lax.dot_general(a, jnp.concatenate(b, axis=1), (((1,), (1,)), ((), ())),
                                    preferred_element_type=F32)
            for u in range(units):
                for oa in range(OFFSETS):
                    k = u * OFFSETS + oa
                    mg[HERE, oa, v:v + 1, pl.ds(u * full, full)] = found[k:k + 1]

    inputs = [
        pltpu.make_async_copy(src, dst, in_sem.at[k]) for k, (src, dst) in enumerate((
            (x_hbm, xg.at[HERE]), (expert_hbm, expert_ref), (slot_hbm, slot_ref), (gate_hbm, gate_ref)))]
    with scope("enter"):
        go(inputs)
        barrier = pltpu.get_barrier_semaphore()
        peers = [at(da, db, j) for da, db in ((1, 0), (-1, 0), (0, 1), (0, -1)) for j in (SAME, OTHER)]
        peers.append(at(0, 0, OTHER))
        for peer in peers:
            pl.semaphore_signal(barrier, inc=1, device_id={"ep": peer}, device_id_type=MESH)
    with scope("x_in"):
        done(inputs)
        for t in range(ahead):
            go(up_tile(0, t))
        pl.semaphore_wait(barrier, len(peers))
        start(("x", ON, 0), ("x", BACK, 0))
    with scope("routing"):
        routing()
        if full > unit:
            r[:, pl.ds(unit, full - unit), :] = jnp.zeros((units, full - unit, d), BF16)
        start(("m", FAR), ("x", ON, 1), ("x", BACK, 1), ("m", ON), ("m", BACK))

    with scope("shared_up"):
        ups(0, lambda e: xg[HERE])

    def shared_store(cols, first, second):
        ysh[:, cols] = first + second

    with scope("x_wait"):
        for i in (ON, BACK):
            arrived(("x", i, 0))
            start(("xx", i))
    with scope("shared_down"):
        downs(0, shared_store)
    with scope("wait_mm"):
        arrived(("m", FAR))
        start("mm")
    with scope("x_rest"):
        for i in (ON, BACK):
            arrived(("x", i, 1), ("m", i))

    def table(s, v=0):
        return mg[s, s, v:v + 1, :]

    def tables(sources):
        merged = jnp.zeros((2 * OFFSETS, total), F32)
        row = lax.broadcasted_iota(jnp.int32, merged.shape, 0)
        for s in sources:
            merged = jnp.where(row == s, table(s), merged)
        column[...] = jnp.transpose(merged)

    step = min(d, 8 * LANE)

    def gather(i, j, out, end=OFFSETS):
        begin = index[i, j] * full
        lane = lax.broadcasted_iota(jnp.int32, (unit, tokens), 1).astype(F32) + 1.0
        for s in range(end):
            token = column[pl.ds(begin, unit), s:s + 1]
            onehot[:, pl.ds(s * tokens, tokens)] = jnp.where(lane == token, 1.0, 0.0).astype(BF16)
        these = pl.ds(0, end * tokens)

        @pl.loop(0, d // step)
        def _(k):
            cols = pl.ds(pl.multiple_of(k * step, step), step)
            out[:, cols] = dot(onehot[:, these], xg[:end, :, cols].reshape(end * tokens, step)).astype(BF16)

    def gather_far(i, j, out):
        begin, late = index[i, j] * full, spans[free:]
        token = jnp.concatenate(
            [column[pl.ds(begin + first, end - first), FAR:FAR + 1] for first, end in late], axis=0)
        lane = lax.broadcasted_iota(jnp.int32, (token.shape[0], tokens), 1).astype(F32) + 1.0
        onehot[pl.ds(0, token.shape[0]), pl.ds(0, tokens)] = jnp.where(lane == token, 1.0, 0.0).astype(BF16)

        @pl.loop(0, d // step)
        def _(k):
            cols = pl.ds(pl.multiple_of(k * step, step), step)
            v, done_rows = dot(onehot[pl.ds(0, token.shape[0]), pl.ds(0, tokens)], xg[FAR, :, cols]), 0
            for first, end in late:
                n = end - first
                these = pl.ds(first, n)
                out[these, cols] = (v[done_rows:done_rows + n] + out[these, cols].astype(F32)).astype(BF16)
                done_rows += n

    with scope("gather_early"):
        tables((HERE, ON, BACK))
        for i, j in early:
            gather(i, j, sent.at[i, j], end=FAR)
            start(*(("s", i, j, k) for k in range(free)))
    with scope("xx_wait"):
        arrived(("xx", ON), ("xx", BACK), "mm")
    with scope("tables"):
        tables(range(OFFSETS))
    for i, j in early:
        with scope("gather_far"):
            gather_far(i, j, sent.at[i, j])
        start(*(("s", i, j, k) for k in range(free, len(spans))))
    with scope("gather"):
        gather(HERE, OTHER, sent.at[HERE, OTHER])
        start(("s", HERE, OTHER))
        gather(HERE, SAME, z.at[SAME, HERE])
        gather(ON, OTHER, sent.at[ON, OTHER])
        gather(BACK, OTHER, sent.at[BACK, OTHER])

    def all_of(i, j):
        return [("s", i, j, k) for k in range(len(spans))]

    with scope("wait_here"):
        arrived(("s", HERE, OTHER))
    with scope("ffn_here_up"):
        expert_ups(1, (SAME, HERE), (OTHER, HERE))
    with scope("wait_f"):
        for j in (SAME, OTHER):
            arrived(*all_of(FAR, j))
            start(("z", FAR, j))
    start(("s", ON, OTHER), ("s", BACK, OTHER))
    with scope("ffn_here_down"):
        expert_downs(1, r.at[index[HERE, SAME]], z.at[OTHER, HERE])
    start(("r", HERE, OTHER))
    with scope("weigh"):
        before = [("x", i, k) for i in (ON, BACK) for k in range(2)] + [("xx", ON), ("xx", BACK)]
        for name in before:
            c[name].wait_send()
        for s in range(OFFSETS):
            token = lax.broadcasted_iota(jnp.int32, (tokens, total), 0).astype(F32) + 1.0
            xg[s] = jnp.where(token == table(s), table(s, 1), 0.0).astype(BF16)
    with scope("wait_same"):
        arrived(*all_of(ON, SAME), *all_of(BACK, SAME))
    with scope("ffn_same"):
        expert_ups(2, (SAME, ON), (SAME, BACK))
        expert_downs(2, z.at[SAME, ON], z.at[SAME, BACK])
    start(("r", ON, SAME), ("r", BACK, SAME))
    with scope("wait_far"):
        arrived(("z", FAR, SAME), ("z", FAR, OTHER))
    with scope("ffn_far"):
        expert_ups(3, (SAME, FAR), (OTHER, FAR))
        for v in range(2):
            expert_downs(3, z.at[SAME, FAR], z.at[OTHER, FAR], v * n_down // 4, (v + 1) * n_down // 4)
            start(("g", SAME, v), ("g", OTHER, v))
    with scope("wait_other"):
        arrived(("s", ON, OTHER), ("s", BACK, OTHER))
    with scope("ffn_other"):
        expert_ups(4, (OTHER, ON), (OTHER, BACK))
        for v in range(2):
            expert_downs(4, z.at[OTHER, ON], z.at[OTHER, BACK], v * n_down // 4, (v + 1) * n_down // 4)
            if v == 0:
                start(("r", ON, OTHER, v), ("r", BACK, OTHER, v))
    with scope("wait_g"):
        for v in range(2):
            for j in (SAME, OTHER):
                arrived(("g", j, v))
                start(("r", FAR, j, v))
            if v == 0:
                start(("r", ON, OTHER, 1), ("r", BACK, OTHER, 1))

    def add_up(s, v, first=0, end=units):
        cols = sides[v]
        these = pl.ds(first * full, (end - first) * full)
        return dot(xg[s, :, these], r[first:end, :, cols].reshape((end - first) * full, d // 2))

    with scope("wait_r_same"):
        arrived(("r", HERE, OTHER), ("r", ON, SAME), ("r", BACK, SAME))
    for v, cols in enumerate(sides):
        with scope("wait_r_other"):
            arrived(("r", ON, OTHER, v), ("r", BACK, OTHER, v))
        with scope("sum_far_early"):
            o = add_up(FAR, v, end=index[FAR, SAME])
            near[0, :, cols] = o[:half]
            near[1, :, cols] = o[half:]
        with scope("wait_r_far"):
            arrived(("r", FAR, SAME, v), ("r", FAR, OTHER, v))
        with scope("sum_far"):
            o = add_up(FAR, v, first=index[FAR, SAME])
            part[2, lo, cols] = (near[0, :, cols] + o[:half]).astype(BF16)
            part[2, hi, cols] = (near[1, :, cols] + o[half:]).astype(BF16)
        start(("pp", 0, v), ("pp", 1, v))
        with scope("sum_near"):
            o = add_up(BACK, v)
            near[0, :, cols] = o[:half]
            part[0, hi, cols] = o[half:].astype(BF16)
            start(("p", 0, 0, v))
            o = add_up(ON, v)
            near[1, :, cols] = o[half:]
            part[1, lo, cols] = o[:half].astype(BF16)
            start(("p", 1, 0, v))
        with scope("sum_own"):
            ysh[:, cols] = ysh[:, cols] + add_up(HERE, v)
        with scope("wait_pp"):
            for k, first in ((0, lo), (1, hi)):
                arrived(("pp", k, v))
                part[k, first, cols] = (near[k, :, cols] + rfar[k, :, cols].astype(F32)).astype(BF16)
                start(("p", k, 1, v))
    outputs = []
    for v, cols in enumerate(sides):
        with scope("wait_p"):
            arrived(*(("p", k, n, v) for k in range(2) for n in range(2)))
        with scope("leave"):
            y = ysh[:, cols] + (rn[0, :, cols].astype(F32) + rn[1, :, cols].astype(F32))
            ybuf[:, cols] = y.astype(BF16)
            outputs.append(pltpu.make_async_copy(ybuf.at[:, cols], y_hbm.at[:, cols], in_sem.at[4 + v]))
            go(outputs[v:])
    with scope("end"):
        for name, one in c.items():
            if name not in before:
                one.wait_send()
        done(outputs)


def solution(mesh):
    side = math.isqrt(mesh.shape["ep"] // 2)
    assert side == OFFSETS

    def local(x, expert, slot, gate, w_gate, w_up, w_down, s_gate, s_up, s_down):
        tokens, d = x.shape[2:]
        top = expert.shape[3]
        per, _, ff = w_gate.shape
        experts = per * mesh.shape["ep"]
        slots = 5 * tokens * top // (4 * experts)
        unit = per * OFFSETS * slots
        full = unit + (-unit) % LANE
        half, units = tokens // 2, len(UNITS)
        choices = (v.transpose(0, 3, 1, 2).reshape(top, 1, tokens) for v in (expert, slot, gate))
        anywhere = pl.BlockSpec(memory_space=pl.ANY)
        y = pl.pallas_call(
            functools.partial(kernel, side, slots),
            out_shape=jax.ShapeDtypeStruct((tokens, d), x.dtype),
            in_specs=[anywhere] * 10,
            out_specs=anywhere,
            scratch_shapes=[
                *(pltpu.VMEM((top, 1, tokens), v.dtype) for v in (expert, slot, gate)),
                pltpu.VMEM((OFFSETS, tokens, d), BF16),
                pltpu.VMEM((OFFSETS, OFFSETS, 2, units * full), F32),
                pltpu.VMEM((units * full, 2 * OFFSETS), F32),
                pltpu.VMEM((unit, OFFSETS * tokens), BF16),
                pltpu.VMEM((tokens, d), BF16),
                pltpu.VMEM((OFFSETS, 2, unit, d), BF16),
                pltpu.VMEM((2, unit, d), BF16),
                pltpu.VMEM((2, OFFSETS, unit, d), BF16),
                pltpu.VMEM((units, full, d), BF16),
                pltpu.VMEM((2, unit, d), BF16),
                pltpu.VMEM((per, 2 * (unit // per + 8), ff), BF16),
                pltpu.VMEM((BUFFERS, per, d, WIDE), BF16),
                pltpu.VMEM((3, tokens, d), BF16),
                pltpu.VMEM((2, half, d), F32),
                pltpu.VMEM((2, half, d), BF16),
                pltpu.VMEM((2, tokens, d), BF16),
                pltpu.VMEM((tokens, d), F32),
                pltpu.SemaphoreType.DMA((6,)),
                pltpu.SemaphoreType.DMA((BUFFERS, 4)),
                pltpu.SemaphoreType.DMA((COPIES,)),
                pltpu.SemaphoreType.DMA((COPIES,)),
            ],
            compiler_params=pltpu.CompilerParams(
                collective_id=0, has_side_effects=True, vmem_limit_bytes=67_000_000),
            name="moe",
        )(x.reshape(tokens, d), *choices, w_gate, w_up, w_down, s_gate, s_up, s_down)
        return y.reshape(x.shape)

    spread, held, whole = P("dp", "ep", None, None), P("ep", None, None), P(None, None)
    return jax.shard_map(
        local, mesh=mesh, in_specs=(spread,) * 4 + (held,) * 3 + (whole,) * 3, out_specs=spread, check_vma=False)
```

```python
import contextlib
import functools
import math

import jax
import jax.numpy as jnp
from jax import lax
from jax.experimental import pallas as pl
from jax.experimental.pallas import tpu as pltpu
from jax.sharding import PartitionSpec as P

MESH = pl.DeviceIdType.MESH
OFFSETS = 4
HERE, ON, BACK, FAR = range(OFFSETS)
SAME, OTHER = range(2)
UNITS = ((HERE, SAME), (HERE, OTHER), (ON, SAME), (BACK, SAME), (ON, OTHER), (BACK, OTHER), (FAR, SAME), (FAR, OTHER))
LANE = 128
WIDE = 2 * LANE
BUFFERS = 6
SENDS, LANDINGS = 9, 25
BF16, F32 = jnp.bfloat16, jnp.float32
scope = contextlib.nullcontext


def dot(a, b):
    return jnp.dot(a, b, preferred_element_type=F32)


def swiglu(both):
    g, u = both[:, :LANE], both[:, LANE:]
    return (g * jax.nn.sigmoid(g) * u).astype(BF16)


def kernel(side, slots, x_hbm, expert_hbm, slot_hbm, gate_hbm, wg, wu, wd, sg, su, sd, y_ref,
           expert_ref, slot_ref, gate_ref, xg, mg, column, onehot, sent, fwd, z, r, fwdb, h, w, part, near, rfar, rn, ysh,
           in_sem, w_sem, send_sem, recv_sem):
    tokens, d = x_hbm.shape
    per, _, ff = wg.shape
    group = OFFSETS * slots
    unit = per * group
    rows = group + (-group) % 16
    last = unit - rows
    half = tokens // 2
    full = unit + (-unit) % LANE
    units = len(UNITS)
    total = units * full
    index = {u: k for k, u in enumerate(UNITS)}

    me = lax.axis_index("ep")
    core, chip = lax.rem(me, 2), lax.div(me, 2)
    py, px = lax.rem(chip, side), lax.div(chip, side)
    pa, pb = px + (py - px) * core, py + (px - py) * core
    sa, sb = 2 * side - (2 * side - 2) * core, 2 + (2 * side - 2) * core

    def at(da, db, other):
        a, b = lax.rem(pa + da + side, side), lax.rem(pb + db + side, side)
        return sa * a + sb * b + (1 - core if other else core)

    lo, hi, body = pl.ds(0, half), pl.ds(half, half), pl.ds(0, unit)
    sides = pl.ds(0, d // 2), pl.ds(d // 2, d // 2)
    spans = [(e * group + (-e * group) % 16, (e * group + FAR * slots) // 16 * 16) for e in range(per)]
    free = len(spans)
    spans += [(spans[e][1], spans[e + 1][0] if e + 1 < per else unit) for e in range(per)]
    assert spans[0][0] == 0
    early = ((FAR, SAME), (FAR, OTHER), (ON, SAME), (BACK, SAME))
    c, sends, landings = {}, {}, {}

    def link(name, src, dst, to, out, into):
        c[name] = pltpu.make_async_remote_copy(
            src_ref=src, dst_ref=dst, send_sem=send_sem.at[sends.setdefault(out, len(sends))],
            recv_sem=recv_sem.at[landings.setdefault(into, len(landings))],
            device_id={"ep": to}, device_id_type=MESH)

    def back(i, j):
        return r.at[index[i, j], body]

    for i, way, first, second in ((ON, 1, lo, hi), (BACK, -1, hi, lo)):
        link(("x", i, 0), xg.at[HERE, first], xg.at[i, first], at(way, 0, SAME), "x", ("x", i, 0))
        link(("x", i, 1), xg.at[HERE, second], xg.at[i, second], at(way, 0, SAME), "x", ("x", i, 1))
        link(("xx", i), xg.at[i, first], xg.at[FAR, first], at(way, 0, SAME), "x", "xx")
        link(("m", i), mg.at[HERE, i], mg.at[i, i], at(way, 0, SAME), "m", ("m", i))
    link(("m", FAR), mg.at[HERE, FAR], mg.at[ON, FAR], at(1, 0, SAME), "m", ("m", FAR))
    link("mm", mg.at[ON, FAR], mg.at[FAR, FAR], at(1, 0, SAME), "m", "mm")

    def unit_links(i, j, dst, to, out, into):
        if (i, j) in early:
            for k, (first, end) in enumerate(spans):
                these = pl.ds(first, end - first)
                link(("s", i, j, k), sent.at[i, j, these], dst.at[these], to, out, into)
        else:
            link(("s", i, j), sent.at[i, j], dst, to, out, into)

    unit_links(HERE, OTHER, z.at[OTHER, HERE], at(0, 0, OTHER), "s_here", "s_here")
    link(("r", HERE, OTHER), z.at[OTHER, HERE], back(HERE, OTHER), at(0, 0, OTHER), ("z", OTHER), "r")
    for i, way in ((ON, 1), (BACK, -1)):
        for j in (SAME, OTHER):
            unit_links(i, j, z.at[j, i], at(0, way, j), "s", ("s", j))
        link(("r", i, SAME), z.at[SAME, i], back(i, SAME), at(0, -way, SAME), ("z", SAME), "r")
        for v, cols in enumerate(sides):
            link(("r", i, OTHER, v), z.at[OTHER, i, :, cols], back(i, OTHER).at[:, cols], at(-way, 0, OTHER),
                 ("z", OTHER), ("r", OTHER, v))
    for j, way in ((SAME, 1), (OTHER, -1)):
        unit_links(FAR, j, fwd.at[j], at(0, way, SAME), "s", "fwd")
        link(("z", FAR, j), fwd.at[j], z.at[j, FAR], at(0, way, j), "fwd", "z_far")
        for v, cols in enumerate(sides):
            to = at(0, -1, SAME) if j == SAME else at(1, 0, OTHER)
            link(("g", j, v), z.at[j, FAR, :, cols], fwdb.at[j, :, cols], to, ("z", j), ("g", v))
            link(("r", FAR, j, v), fwdb.at[j, :, cols], back(FAR, j).at[:, cols], at(0, -way, SAME),
                 "fwdb", ("r", FAR, v))
    for k, way, first, second in ((0, 1, lo, hi), (1, -1, hi, lo)):
        for v, cols in enumerate(sides):
            link(("pp", k, v), part.at[2, first, cols], rfar.at[k, :, cols], at(way, 0, SAME), "part", ("pp", v))
            for n, these in enumerate((second, first)):
                link(("p", k, n, v), part.at[k, these, cols], rn.at[k, these, cols], at(way, 0, SAME),
                     "part", ("p", v))
    assert len(sends) == SENDS and len(landings) == LANDINGS

    def start(*which):
        for i in which:
            c[i].start()

    def wait(sem, ref):
        pltpu.make_async_copy(ref, ref, sem).wait()

    def arrived(into, ref):
        wait(recv_sem.at[landings[into]], ref)

    def gone(out, ref):
        wait(send_sem.at[sends[out]], ref)

    near_units = pl.ds(index[HERE, OTHER], 3)
    other_units, far_units = pl.ds(index[ON, OTHER], 2), pl.ds(index[FAR, SAME], 2)

    n_up, n_down, passes = ff // LANE, d // WIDE, 5
    n_tiles = n_up + n_down
    ahead = BUFFERS - 2
    assert per == 2 and n_up % 2 == 1 and n_down % 2 == 0

    def slot_of(p, t):
        return lax.rem(p * n_tiles + t, BUFFERS)

    def up_tile(p, t):
        slot = slot_of(p, t)
        out = []
        for e in range(per):
            for k, (shared, own) in enumerate(((sg, wg), (su, wu))):
                if p == 0:
                    src = shared.at[:, pl.ds(pl.multiple_of(e * ff + t * LANE, LANE), LANE)]
                else:
                    src = own.at[e, :, pl.ds(pl.multiple_of(t * LANE, LANE), LANE)]
                out.append(pltpu.make_async_copy(
                    src, w.at[slot, e, :, pl.ds(k * LANE, LANE)], w_sem.at[slot]))
        return out

    def down_tile(p, t):
        slot = slot_of(p, t)
        cols = pl.ds(pl.multiple_of((t - n_up) * WIDE, WIDE), WIDE)
        out = []
        for e in range(per):
            src = sd.at[pl.ds(e * ff, ff), cols] if p == 0 else wd.at[e, :, cols]
            out.append(pltpu.make_async_copy(src, w.at[slot, e, pl.ds(0, ff), :], w_sem.at[slot]))
        return out

    def go(copies):
        for one in copies:
            one.start()

    def done(copies):
        for one in copies:
            one.wait()

    def fetch_in_up(p, q):
        @pl.when(q < n_up)
        def _():
            go(up_tile(p, q))

        @pl.when(q >= n_up)
        def _():
            go(down_tile(p, q))

    def fetch_in_down(p, q):
        @pl.when(q < n_tiles)
        def _():
            go(down_tile(p, q))

        if p + 1 < passes:
            @pl.when(q >= n_tiles)
            def _():
                go(up_tile(p + 1, q - n_tiles))

    def ups(p, lhs):
        def some(ts):
            for t in ts:
                slot = slot_of(p, t)
                wait(w_sem.at[slot], w.at[slot])
            for t in ts:
                fetch_in_up(p, t + ahead)
            for t in ts:
                for e in range(per):
                    v = swiglu(dot(lhs(e), w[slot_of(p, t), e]))
                    h[e, :, pl.ds(pl.multiple_of(t * LANE, LANE), LANE)] = v

        @pl.loop(0, n_up // 2)
        def _(i):
            some((2 * i, 2 * i + 1))

        some((jnp.int32(n_up - 1),))

    def downs(p, store, begin=0, end=n_down // 2):
        @pl.loop(begin, end)
        def _(i):
            ts = (n_up + 2 * i, n_up + 2 * i + 1)
            for t in ts:
                slot = slot_of(p, t)
                wait(w_sem.at[slot], w.at[slot, :, pl.ds(0, ff), :])
            for t in ts:
                fetch_in_down(p, t + ahead)
            for t in ts:
                cols = pl.ds(pl.multiple_of((t - n_up) * WIDE, WIDE), WIDE)
                store(cols, *(dot(h[e], w[slot_of(p, t), e, pl.ds(0, ff), :]) for e in range(per)))

    def expert_ups(p, a, b):
        def lhs(e):
            these = pl.ds(e * last, rows)
            return jnp.concatenate([z[*a, these, :], z[*b, these, :]], axis=0)
        ups(p, lhs)

    def expert_downs(p, a, b, *which):
        def store(cols, first, second):
            for k, ref in enumerate((a, b)):
                v, u = (o[k * rows:(k + 1) * rows] for o in (first, second))
                row = lax.broadcasted_iota(jnp.int32, (rows - last, WIDE), 0)
                edge = jnp.where(row < group - last, v[last:], u[:rows - last])
                ref[pl.ds(0, last), cols] = v[:last].astype(BF16)
                ref[pl.ds(last, rows - last), cols] = edge.astype(BF16)
                ref[pl.ds(rows, last), cols] = u[rows - last:].astype(BF16)
        downs(p, store, *which)

    def routing():
        def place(to, here):
            away = lax.rem(to - here + side, side)
            return away ^ lax.shift_right_logical(away, 1)

        tos, spots, numbers = [], [], []
        number = lax.broadcasted_iota(jnp.int32, (1, tokens), 1).astype(F32) + 1.0
        n_to = OFFSETS * units
        for k in range(expert_ref.shape[0]):
            expert, slot = expert_ref[k], slot_ref[k]
            device, e = lax.div(expert, per), lax.rem(expert, per)
            other = lax.rem(device, 2) ^ core
            chip_to = lax.div(device, 2)
            ty, tx = lax.rem(chip_to, side), lax.div(chip_to, side)
            ta, tb = tx + (ty - tx) * core, ty + (tx - ty) * core
            oa, ob = place(ta, pa), place(tb, pb)
            u = jnp.where(ob == HERE, other, jnp.where(ob == FAR, index[FAR, SAME] + other, ob + 1 + 2 * other))
            to = u * OFFSETS + oa
            spot = jnp.where(slot < slots, (e * OFFSETS + oa) * slots + slot, -1)
            tos.append(jnp.where(lax.broadcasted_iota(jnp.int32, (n_to, tokens), 0) == to, 1.0, 0.0).astype(BF16))
            hit = lax.broadcasted_iota(jnp.int32, (full, tokens), 0) == spot
            spots.append(jnp.where(hit, number, 0.0).astype(BF16))
            numbers.append(jnp.where(hit, gate_ref[k], 0.0).astype(BF16))
        a = jnp.concatenate(tos, axis=1)
        for v, b in enumerate((spots, numbers)):
            found = lax.dot_general(a, jnp.concatenate(b, axis=1), (((1,), (1,)), ((), ())),
                                    preferred_element_type=F32)
            for u in range(units):
                for oa in range(OFFSETS):
                    k = u * OFFSETS + oa
                    mg[HERE, oa, v:v + 1, pl.ds(u * full, full)] = found[k:k + 1]

    inputs = [
        pltpu.make_async_copy(src, dst, in_sem.at[k]) for k, (src, dst) in enumerate((
            (x_hbm, xg.at[HERE]), (expert_hbm, expert_ref), (slot_hbm, slot_ref), (gate_hbm, gate_ref)))]
    with scope("enter"):
        go(inputs)
        barrier = pltpu.get_barrier_semaphore()
        peers = [at(da, db, j) for da, db in ((1, 0), (-1, 0), (0, 1), (0, -1)) for j in (SAME, OTHER)]
        peers.append(at(0, 0, OTHER))
        for peer in peers:
            pl.semaphore_signal(barrier, inc=1, device_id={"ep": peer}, device_id_type=MESH)
    with scope("x_in"):
        done(inputs)
        for t in range(ahead):
            go(up_tile(0, t))
        pl.semaphore_wait(barrier, len(peers))
        start(("x", ON, 0), ("x", BACK, 0))
    with scope("routing"):
        routing()
        if full > unit:
            r[:, pl.ds(unit, full - unit), :] = jnp.zeros((units, full - unit, d), BF16)
        start(("m", FAR), ("x", ON, 1), ("x", BACK, 1), ("m", ON), ("m", BACK))

    with scope("shared_up"):
        ups(0, lambda e: xg[HERE])

    def shared_store(cols, first, second):
        ysh[:, cols] = first + second

    with scope("x_wait"):
        for i, first in ((ON, lo), (BACK, hi)):
            arrived(("x", i, 0), xg.at[i, first])
            start(("xx", i))
    with scope("shared_down"):
        downs(0, shared_store)
    with scope("wait_mm"):
        arrived(("m", FAR), mg.at[ON, FAR])
        start("mm")
    with scope("x_rest"):
        for i, second in ((ON, hi), (BACK, lo)):
            arrived(("x", i, 1), xg.at[i, second])
            arrived(("m", i), mg.at[i, i])

    def table(s, v=0):
        return mg[s, s, v:v + 1, :]

    def tables(sources):
        merged = jnp.zeros((2 * OFFSETS, total), F32)
        row = lax.broadcasted_iota(jnp.int32, merged.shape, 0)
        for s in sources:
            merged = jnp.where(row == s, table(s), merged)
        column[...] = jnp.transpose(merged)

    step = min(d, 8 * LANE)

    def gather(i, j, out, end=OFFSETS):
        begin = index[i, j] * full
        lane = lax.broadcasted_iota(jnp.int32, (unit, tokens), 1).astype(F32) + 1.0
        for s in range(end):
            token = column[pl.ds(begin, unit), s:s + 1]
            onehot[:, pl.ds(s * tokens, tokens)] = jnp.where(lane == token, 1.0, 0.0).astype(BF16)
        these = pl.ds(0, end * tokens)

        @pl.loop(0, d // step)
        def _(k):
            cols = pl.ds(pl.multiple_of(k * step, step), step)
            out[:, cols] = dot(onehot[:, these], xg[:end, :, cols].reshape(end * tokens, step)).astype(BF16)

    def gather_far(i, j, out):
        begin, late = index[i, j] * full, spans[free:]
        token = jnp.concatenate(
            [column[pl.ds(begin + first, end - first), FAR:FAR + 1] for first, end in late], axis=0)
        lane = lax.broadcasted_iota(jnp.int32, (token.shape[0], tokens), 1).astype(F32) + 1.0
        onehot[pl.ds(0, token.shape[0]), pl.ds(0, tokens)] = jnp.where(lane == token, 1.0, 0.0).astype(BF16)

        @pl.loop(0, d // step)
        def _(k):
            cols = pl.ds(pl.multiple_of(k * step, step), step)
            v, done_rows = dot(onehot[pl.ds(0, token.shape[0]), pl.ds(0, tokens)], xg[FAR, :, cols]), 0
            for first, end in late:
                n = end - first
                these = pl.ds(first, n)
                out[these, cols] = (v[done_rows:done_rows + n] + out[these, cols].astype(F32)).astype(BF16)
                done_rows += n

    with scope("gather_early"):
        tables((HERE, ON, BACK))
        for i, j in early:
            gather(i, j, sent.at[i, j], end=FAR)
            start(*(("s", i, j, k) for k in range(free)))
    with scope("xx_wait"):
        arrived("xx", xg.at[FAR])
        arrived("mm", mg.at[FAR, FAR])
    with scope("tables"):
        tables(range(OFFSETS))
    for i, j in early:
        with scope("gather_far"):
            gather_far(i, j, sent.at[i, j])
        start(*(("s", i, j, k) for k in range(free, len(spans))))
    with scope("gather"):
        gather(HERE, OTHER, sent.at[HERE, OTHER])
        start(("s", HERE, OTHER))
        gather(HERE, SAME, z.at[SAME, HERE])
        gather(ON, OTHER, sent.at[ON, OTHER])
        gather(BACK, OTHER, sent.at[BACK, OTHER])

    with scope("wait_here"):
        arrived("s_here", z.at[OTHER, HERE])
    with scope("ffn_here_up"):
        expert_ups(1, (SAME, HERE), (OTHER, HERE))
    with scope("wait_f"):
        arrived("fwd", fwd)
        start(("z", FAR, SAME), ("z", FAR, OTHER))
    start(("s", ON, OTHER), ("s", BACK, OTHER))
    with scope("ffn_here_down"):
        expert_downs(1, r.at[index[HERE, SAME]], z.at[OTHER, HERE])
    start(("r", HERE, OTHER))
    with scope("weigh"):
        gone("x", xg.at[pl.ds(0, 3)])
        for s in range(OFFSETS):
            token = lax.broadcasted_iota(jnp.int32, (tokens, total), 0).astype(F32) + 1.0
            xg[s] = jnp.where(token == table(s), table(s, 1), 0.0).astype(BF16)
    with scope("wait_same"):
        arrived(("s", SAME), z.at[SAME, pl.ds(ON, 2)])
    with scope("ffn_same"):
        expert_ups(2, (SAME, ON), (SAME, BACK))
        expert_downs(2, z.at[SAME, ON], z.at[SAME, BACK])
    start(("r", ON, SAME), ("r", BACK, SAME))
    with scope("wait_far"):
        arrived("z_far", z.at[:, FAR])
    with scope("ffn_far"):
        expert_ups(3, (SAME, FAR), (OTHER, FAR))
        for v in range(2):
            expert_downs(3, z.at[SAME, FAR], z.at[OTHER, FAR], v * n_down // 4, (v + 1) * n_down // 4)
            start(("g", SAME, v), ("g", OTHER, v))
    with scope("wait_other"):
        arrived(("s", OTHER), z.at[OTHER, pl.ds(ON, 2)])
    with scope("ffn_other"):
        expert_ups(4, (OTHER, ON), (OTHER, BACK))
        for v in range(2):
            expert_downs(4, z.at[OTHER, ON], z.at[OTHER, BACK], v * n_down // 4, (v + 1) * n_down // 4)
            if v == 0:
                start(("r", ON, OTHER, v), ("r", BACK, OTHER, v))
    with scope("wait_g"):
        for v, cols in enumerate(sides):
            arrived(("g", v), fwdb.at[:, :, cols])
            start(("r", FAR, SAME, v), ("r", FAR, OTHER, v))
            if v == 0:
                start(("r", ON, OTHER, 1), ("r", BACK, OTHER, 1))

    def add_up(s, v, first=0, end=units):
        cols = sides[v]
        these = pl.ds(first * full, (end - first) * full)
        return dot(xg[s, :, these], r[first:end, :, cols].reshape((end - first) * full, d // 2))

    with scope("wait_r_same"):
        arrived("r", r.at[near_units, body])
    for v, cols in enumerate(sides):
        with scope("wait_r_other"):
            arrived(("r", OTHER, v), r.at[other_units, body, cols])
        with scope("sum_far_early"):
            o = add_up(FAR, v, end=index[FAR, SAME])
            near[0, :, cols] = o[:half]
            near[1, :, cols] = o[half:]
        with scope("wait_r_far"):
            arrived(("r", FAR, v), r.at[far_units, body, cols])
        with scope("sum_far"):
            o = add_up(FAR, v, first=index[FAR, SAME])
            part[2, lo, cols] = (near[0, :, cols] + o[:half]).astype(BF16)
            part[2, hi, cols] = (near[1, :, cols] + o[half:]).astype(BF16)
        start(("pp", 0, v), ("pp", 1, v))
        with scope("sum_near"):
            o = add_up(BACK, v)
            near[0, :, cols] = o[:half]
            part[0, hi, cols] = o[half:].astype(BF16)
            start(("p", 0, 0, v))
            o = add_up(ON, v)
            near[1, :, cols] = o[half:]
            part[1, lo, cols] = o[:half].astype(BF16)
            start(("p", 1, 0, v))
        with scope("sum_own"):
            ysh[:, cols] = ysh[:, cols] + add_up(HERE, v)
        with scope("wait_pp"):
            arrived(("pp", v), rfar.at[:, :, cols])
            for k, first in ((0, lo), (1, hi)):
                part[k, first, cols] = (near[k, :, cols] + rfar[k, :, cols].astype(F32)).astype(BF16)
                start(("p", k, 1, v))
    for v, cols in enumerate(sides):
        with scope("wait_p"):
            arrived(("p", v), rn.at[:, :, cols])
        with scope("leave"):
            y = ysh[:, cols] + (rn[0, :, cols].astype(F32) + rn[1, :, cols].astype(F32))
            y_ref[:, cols] = y.astype(y_ref.dtype)
    with scope("end"):
        gone("m", mg.at[HERE])
        gone("s_here", sent.at[HERE, OTHER])
        gone("s", sent.at[pl.ds(ON, 3)])
        gone("fwd", fwd)
        gone(("z", SAME), z.at[SAME, pl.ds(ON, 3)])
        gone(("z", OTHER), z.at[OTHER])
        gone("fwdb", fwdb)
        gone("part", part)


def solution(mesh):
    side = math.isqrt(mesh.shape["ep"] // 2)
    assert side == OFFSETS

    def local(x, expert, slot, gate, w_gate, w_up, w_down, s_gate, s_up, s_down):
        tokens, d = x.shape[2:]
        top = expert.shape[3]
        per, _, ff = w_gate.shape
        experts = per * mesh.shape["ep"]
        slots = 5 * tokens * top // (4 * experts)
        unit = per * OFFSETS * slots
        full = unit + (-unit) % LANE
        half, units = tokens // 2, len(UNITS)
        choices = (v.transpose(0, 3, 1, 2).reshape(top, 1, tokens) for v in (expert, slot, gate))
        anywhere = pl.BlockSpec(memory_space=pl.ANY)
        y = pl.pallas_call(
            functools.partial(kernel, side, slots),
            out_shape=pltpu.VMEM((tokens, d), x.dtype),
            in_specs=[anywhere] * 10,
            out_specs=pl.BlockSpec(memory_space=pltpu.VMEM),
            scratch_shapes=[
                *(pltpu.VMEM((top, 1, tokens), v.dtype) for v in (expert, slot, gate)),
                pltpu.VMEM((OFFSETS, tokens, d), BF16),
                pltpu.VMEM((OFFSETS, OFFSETS, 2, units * full), F32),
                pltpu.VMEM((units * full, 2 * OFFSETS), F32),
                pltpu.VMEM((unit, OFFSETS * tokens), BF16),
                pltpu.VMEM((OFFSETS, 2, unit, d), BF16),
                pltpu.VMEM((2, unit, d), BF16),
                pltpu.VMEM((2, OFFSETS, unit, d), BF16),
                pltpu.VMEM((units, full, d), BF16),
                pltpu.VMEM((2, unit, d), BF16),
                pltpu.VMEM((per, 2 * (unit // per + 8), ff), BF16),
                pltpu.VMEM((BUFFERS, per, d, WIDE), BF16),
                pltpu.VMEM((3, tokens, d), BF16),
                pltpu.VMEM((2, half, d), F32),
                pltpu.VMEM((2, half, d), BF16),
                pltpu.VMEM((2, tokens, d), BF16),
                pltpu.VMEM((tokens, d), F32),
                pltpu.SemaphoreType.DMA((4,)),
                pltpu.SemaphoreType.DMA((BUFFERS,)),
                pltpu.SemaphoreType.DMA((SENDS,)),
                pltpu.SemaphoreType.DMA((LANDINGS,)),
            ],
            compiler_params=pltpu.CompilerParams(
                collective_id=0, has_side_effects=True, vmem_limit_bytes=62_500_000),
            name="moe",
        )(x.reshape(tokens, d), *choices, w_gate, w_up, w_down, s_gate, s_up, s_down)
        return y.reshape(x.shape)

    spread, held, whole = P("dp", "ep", None, None), P("ep", None, None), P(None, None)
    return jax.shard_map(
        local, mesh=mesh, in_specs=(spread,) * 4 + (held,) * 3 + (whole,) * 3, out_specs=spread, check_vma=False)
```

```python
import contextlib
import functools
import math

import jax
import jax.numpy as jnp
from jax import lax
from jax.experimental import pallas as pl
from jax.experimental.pallas import tpu as pltpu
from jax.sharding import PartitionSpec as P

MESH = pl.DeviceIdType.MESH
OFFSETS = 4
HERE, ON, BACK, FAR = range(OFFSETS)
SAME, OTHER = range(2)
UNITS = ((HERE, SAME), (HERE, OTHER), (ON, SAME), (BACK, SAME), (ON, OTHER), (BACK, OTHER), (FAR, SAME), (FAR, OTHER))
LANE = 128
WIDE = 2 * LANE
BUFFERS = 7
SENDS, LANDINGS = 9, 25
BF16, F32 = jnp.bfloat16, jnp.float32
scope = contextlib.nullcontext


def dot(a, b):
    return jnp.dot(a, b, preferred_element_type=F32)


def swiglu(both):
    g, u = both[:, :LANE], both[:, LANE:]
    return (g * jax.nn.sigmoid(g) * u).astype(BF16)


def kernel(side, slots, x_hbm, expert_hbm, slot_hbm, gate_hbm, wg, wu, wd, sg, su, sd, y_ref,
           expert_ref, slot_ref, gate_ref, xg, mg, column, onehot, sent, fwd, z, r, fwdb, h, w, part, near, rfar, rn, ysh,
           in_sem, w_sem, send_sem, recv_sem):
    tokens, d = x_hbm.shape
    per, _, ff = wg.shape
    group = OFFSETS * slots
    unit = per * group
    rows = group + (-group) % 16
    last = unit - rows
    half = tokens // 2
    full = unit + (-unit) % LANE
    units = len(UNITS)
    total = units * full
    index = {u: k for k, u in enumerate(UNITS)}

    me = lax.axis_index("ep")
    core, chip = lax.rem(me, 2), lax.div(me, 2)
    py, px = lax.rem(chip, side), lax.div(chip, side)
    pa, pb = px + (py - px) * core, py + (px - py) * core
    sa, sb = 2 * side - (2 * side - 2) * core, 2 + (2 * side - 2) * core

    def at(da, db, other):
        a, b = lax.rem(pa + da + side, side), lax.rem(pb + db + side, side)
        return sa * a + sb * b + (1 - core if other else core)

    lo, hi, body = pl.ds(0, half), pl.ds(half, half), pl.ds(0, unit)
    sides = pl.ds(0, d // 2), pl.ds(d // 2, d // 2)
    spans = [(e * group + (-e * group) % 16, (e * group + FAR * slots) // 16 * 16) for e in range(per)]
    free = len(spans)
    spans += [(spans[e][1], spans[e + 1][0] if e + 1 < per else unit) for e in range(per)]
    assert spans[0][0] == 0
    early = ((FAR, SAME), (FAR, OTHER), (ON, SAME), (BACK, SAME))
    c, sends, landings = {}, {}, {}

    def link(name, src, dst, to, out, into):
        c[name] = pltpu.make_async_remote_copy(
            src_ref=src, dst_ref=dst, send_sem=send_sem.at[sends.setdefault(out, len(sends))],
            recv_sem=recv_sem.at[landings.setdefault(into, len(landings))],
            device_id={"ep": to}, device_id_type=MESH)

    def back(i, j):
        return r.at[index[i, j], body]

    for i, way, first, second in ((ON, 1, lo, hi), (BACK, -1, hi, lo)):
        link(("x", i, 0), xg.at[HERE, first], xg.at[i, first], at(way, 0, SAME), "x", ("x", i, 0))
        link(("x", i, 1), xg.at[HERE, second], xg.at[i, second], at(way, 0, SAME), "x", ("x", i, 1))
        link(("xx", i), xg.at[i, first], xg.at[FAR, first], at(way, 0, SAME), "x", "xx")
        link(("m", i), mg.at[HERE, i], mg.at[i, i], at(way, 0, SAME), "m", ("m", i))
    link(("m", FAR), mg.at[HERE, FAR], mg.at[ON, FAR], at(1, 0, SAME), "m", ("m", FAR))
    link("mm", mg.at[ON, FAR], mg.at[FAR, FAR], at(1, 0, SAME), "m", "mm")

    def unit_links(i, j, dst, to, out, into):
        if (i, j) in early:
            for k, (first, end) in enumerate(spans):
                these = pl.ds(first, end - first)
                link(("s", i, j, k), sent.at[i, j, these], dst.at[these], to, out, into)
        else:
            link(("s", i, j), sent.at[i, j], dst, to, out, into)

    unit_links(HERE, OTHER, z.at[OTHER, HERE], at(0, 0, OTHER), "s_here", "s_here")
    link(("r", HERE, OTHER), z.at[OTHER, HERE], back(HERE, OTHER), at(0, 0, OTHER), ("z", OTHER), "r")
    for i, way in ((ON, 1), (BACK, -1)):
        for j in (SAME, OTHER):
            unit_links(i, j, z.at[j, i], at(0, way, j), "s", ("s", j))
        link(("r", i, SAME), z.at[SAME, i], back(i, SAME), at(0, -way, SAME), ("z", SAME), "r")
        for v, cols in enumerate(sides):
            link(("r", i, OTHER, v), z.at[OTHER, i, :, cols], back(i, OTHER).at[:, cols], at(-way, 0, OTHER),
                 ("z", OTHER), ("r", OTHER, v))
    for j, way in ((SAME, 1), (OTHER, -1)):
        unit_links(FAR, j, fwd.at[j], at(0, way, SAME), "s", "fwd")
        link(("z", FAR, j), fwd.at[j], z.at[j, FAR], at(0, way, j), "fwd", "z_far")
        for v, cols in enumerate(sides):
            to = at(0, -1, SAME) if j == SAME else at(1, 0, OTHER)
            link(("g", j, v), z.at[j, FAR, :, cols], fwdb.at[j, :, cols], to, ("z", j), ("g", v))
            link(("r", FAR, j, v), fwdb.at[j, :, cols], back(FAR, j).at[:, cols], at(0, -way, SAME),
                 "fwdb", ("r", FAR, v))
    for k, way, first, second in ((0, 1, lo, hi), (1, -1, hi, lo)):
        for v, cols in enumerate(sides):
            link(("pp", k, v), part.at[2, first, cols], rfar.at[k, :, cols], at(way, 0, SAME), "part", ("pp", v))
            for n, these in enumerate((second, first)):
                link(("p", k, n, v), part.at[k, these, cols], rn.at[k, these, cols], at(way, 0, SAME),
                     "part", ("p", v))
    assert len(sends) == SENDS and len(landings) == LANDINGS

    def start(*which):
        for i in which:
            c[i].start()

    def wait(sem, ref):
        pltpu.make_async_copy(ref, ref, sem).wait()

    def arrived(into, ref):
        wait(recv_sem.at[landings[into]], ref)

    def gone(out, ref):
        wait(send_sem.at[sends[out]], ref)

    near_units = pl.ds(index[HERE, OTHER], 3)
    other_units, far_units = pl.ds(index[ON, OTHER], 2), pl.ds(index[FAR, SAME], 2)

    n_up, n_down, passes = ff // LANE, d // WIDE, 5
    n_tiles = n_up + n_down
    ahead = BUFFERS - 2
    assert per == 2 and n_up % 2 == 1 and n_down % 2 == 0

    def slot_of(p, t):
        return lax.rem(p * n_tiles + t, BUFFERS)

    def up_tile(p, t):
        slot = slot_of(p, t)
        out = []
        for e in range(per):
            for k, (shared, own) in enumerate(((sg, wg), (su, wu))):
                if p == 0:
                    src = shared.at[:, pl.ds(pl.multiple_of(e * ff + t * LANE, LANE), LANE)]
                else:
                    src = own.at[e, :, pl.ds(pl.multiple_of(t * LANE, LANE), LANE)]
                out.append(pltpu.make_async_copy(
                    src, w.at[slot, e, :, pl.ds(k * LANE, LANE)], w_sem.at[slot]))
        return out

    def down_tile(p, t):
        slot = slot_of(p, t)
        cols = pl.ds(pl.multiple_of((t - n_up) * WIDE, WIDE), WIDE)
        out = []
        for e in range(per):
            src = sd.at[pl.ds(e * ff, ff), cols] if p == 0 else wd.at[e, :, cols]
            out.append(pltpu.make_async_copy(src, w.at[slot, e, pl.ds(0, ff), :], w_sem.at[slot]))
        return out

    def go(copies):
        for one in copies:
            one.start()

    def done(copies):
        for one in copies:
            one.wait()

    def fetch_in_up(p, q):
        @pl.when(q < n_up)
        def _():
            go(up_tile(p, q))

        @pl.when(q >= n_up)
        def _():
            go(down_tile(p, q))

    def fetch_in_down(p, q):
        @pl.when(q < n_tiles)
        def _():
            go(down_tile(p, q))

        if p + 1 < passes:
            @pl.when(q >= n_tiles)
            def _():
                go(up_tile(p + 1, q - n_tiles))

    def ups(p, lhs):
        def some(ts):
            for t in ts:
                slot = slot_of(p, t)
                wait(w_sem.at[slot], w.at[slot])
            for t in ts:
                fetch_in_up(p, t + ahead)
            for t in ts:
                for e in range(per):
                    v = swiglu(dot(lhs(e), w[slot_of(p, t), e]))
                    h[e, :, pl.ds(pl.multiple_of(t * LANE, LANE), LANE)] = v

        @pl.loop(0, n_up // 2)
        def _(i):
            some((2 * i, 2 * i + 1))

        some((jnp.int32(n_up - 1),))

    def downs(p, store, begin=0, end=n_down // 2):
        @pl.loop(begin, end)
        def _(i):
            ts = (n_up + 2 * i, n_up + 2 * i + 1)
            for t in ts:
                slot = slot_of(p, t)
                wait(w_sem.at[slot], w.at[slot, :, pl.ds(0, ff), :])
            for t in ts:
                fetch_in_down(p, t + ahead)
            for t in ts:
                cols = pl.ds(pl.multiple_of((t - n_up) * WIDE, WIDE), WIDE)
                store(cols, *(dot(h[e], w[slot_of(p, t), e, pl.ds(0, ff), :]) for e in range(per)))

    def expert_ups(p, a, b):
        def lhs(e):
            these = pl.ds(e * last, rows)
            return jnp.concatenate([z[*a, these, :], z[*b, these, :]], axis=0)
        ups(p, lhs)

    def expert_downs(p, a, b, *which):
        def store(cols, first, second):
            for k, ref in enumerate((a, b)):
                v, u = (o[k * rows:(k + 1) * rows] for o in (first, second))
                row = lax.broadcasted_iota(jnp.int32, (rows - last, WIDE), 0)
                edge = jnp.where(row < group - last, v[last:], u[:rows - last])
                ref[pl.ds(0, last), cols] = v[:last].astype(BF16)
                ref[pl.ds(last, rows - last), cols] = edge.astype(BF16)
                ref[pl.ds(rows, last), cols] = u[rows - last:].astype(BF16)
        downs(p, store, *which)

    def routing():
        def place(to, here):
            away = lax.rem(to - here + side, side)
            return away ^ lax.shift_right_logical(away, 1)

        tos, spots, numbers = [], [], []
        number = lax.broadcasted_iota(jnp.int32, (1, tokens), 1).astype(F32) + 1.0
        n_to = OFFSETS * units
        for k in range(expert_ref.shape[0]):
            expert, slot = expert_ref[k], slot_ref[k]
            device, e = lax.div(expert, per), lax.rem(expert, per)
            other = lax.rem(device, 2) ^ core
            chip_to = lax.div(device, 2)
            ty, tx = lax.rem(chip_to, side), lax.div(chip_to, side)
            ta, tb = tx + (ty - tx) * core, ty + (tx - ty) * core
            oa, ob = place(ta, pa), place(tb, pb)
            u = jnp.where(ob == HERE, other, jnp.where(ob == FAR, index[FAR, SAME] + other, ob + 1 + 2 * other))
            to = u * OFFSETS + oa
            spot = jnp.where(slot < slots, (e * OFFSETS + oa) * slots + slot, -1)
            tos.append(jnp.where(lax.broadcasted_iota(jnp.int32, (n_to, tokens), 0) == to, 1.0, 0.0).astype(BF16))
            hit = lax.broadcasted_iota(jnp.int32, (full, tokens), 0) == spot
            spots.append(jnp.where(hit, number, 0.0).astype(BF16))
            numbers.append(jnp.where(hit, gate_ref[k], 0.0).astype(BF16))
        a = jnp.concatenate(tos, axis=1)
        for v, b in enumerate((spots, numbers)):
            found = lax.dot_general(a, jnp.concatenate(b, axis=1), (((1,), (1,)), ((), ())),
                                    preferred_element_type=F32)
            for u in range(units):
                for oa in range(OFFSETS):
                    k = u * OFFSETS + oa
                    mg[HERE, oa, v:v + 1, pl.ds(u * full, full)] = found[k:k + 1]

    inputs = [
        pltpu.make_async_copy(src, dst, in_sem.at[k]) for k, (src, dst) in enumerate((
            (x_hbm, xg.at[HERE]), (expert_hbm, expert_ref), (slot_hbm, slot_ref), (gate_hbm, gate_ref)))]
    with scope("enter"):
        go(inputs)
        barrier = pltpu.get_barrier_semaphore()
        peers = [at(da, db, j) for da, db in ((1, 0), (-1, 0), (0, 1), (0, -1)) for j in (SAME, OTHER)]
        peers.append(at(0, 0, OTHER))
        for peer in peers:
            pl.semaphore_signal(barrier, inc=1, device_id={"ep": peer}, device_id_type=MESH)
    with scope("x_in"):
        done(inputs)
        for t in range(ahead):
            go(up_tile(0, t))
        pl.semaphore_wait(barrier, len(peers))
        start(("x", ON, 0), ("x", BACK, 0))
    with scope("routing"):
        routing()
        if full > unit:
            r[:, pl.ds(unit, full - unit), :] = jnp.zeros((units, full - unit, d), BF16)
        start(("m", FAR), ("x", ON, 1), ("x", BACK, 1), ("m", ON), ("m", BACK))

    with scope("shared_up"):
        ups(0, lambda e: xg[HERE])

    def shared_store(cols, first, second):
        ysh[:, cols] = first + second

    with scope("x_wait"):
        for i, first in ((ON, lo), (BACK, hi)):
            arrived(("x", i, 0), xg.at[i, first])
            start(("xx", i))
    with scope("shared_down"):
        downs(0, shared_store)
    with scope("wait_mm"):
        arrived(("m", FAR), mg.at[ON, FAR])
        start("mm")
    with scope("x_rest"):
        for i, second in ((ON, hi), (BACK, lo)):
            arrived(("x", i, 1), xg.at[i, second])
            arrived(("m", i), mg.at[i, i])

    def table(s, v=0):
        return mg[s, s, v:v + 1, :]

    def tables(sources):
        merged = jnp.zeros((2 * OFFSETS, total), F32)
        row = lax.broadcasted_iota(jnp.int32, merged.shape, 0)
        for s in sources:
            merged = jnp.where(row == s, table(s), merged)
        column[...] = jnp.transpose(merged)

    step = min(d, 8 * LANE)

    def gather(i, j, out, end=OFFSETS):
        begin = index[i, j] * full
        lane = lax.broadcasted_iota(jnp.int32, (unit, tokens), 1).astype(F32) + 1.0
        for s in range(end):
            token = column[pl.ds(begin, unit), s:s + 1]
            onehot[:, pl.ds(s * tokens, tokens)] = jnp.where(lane == token, 1.0, 0.0).astype(BF16)
        these = pl.ds(0, end * tokens)

        @pl.loop(0, d // step)
        def _(k):
            cols = pl.ds(pl.multiple_of(k * step, step), step)
            out[:, cols] = dot(onehot[:, these], xg[:end, :, cols].reshape(end * tokens, step)).astype(BF16)

    def gather_far(i, j, out):
        begin, late = index[i, j] * full, spans[free:]
        token = jnp.concatenate(
            [column[pl.ds(begin + first, end - first), FAR:FAR + 1] for first, end in late], axis=0)
        lane = lax.broadcasted_iota(jnp.int32, (token.shape[0], tokens), 1).astype(F32) + 1.0
        onehot[pl.ds(0, token.shape[0]), pl.ds(0, tokens)] = jnp.where(lane == token, 1.0, 0.0).astype(BF16)

        @pl.loop(0, d // step)
        def _(k):
            cols = pl.ds(pl.multiple_of(k * step, step), step)
            v, done_rows = dot(onehot[pl.ds(0, token.shape[0]), pl.ds(0, tokens)], xg[FAR, :, cols]), 0
            for first, end in late:
                n = end - first
                these = pl.ds(first, n)
                out[these, cols] = (v[done_rows:done_rows + n] + out[these, cols].astype(F32)).astype(BF16)
                done_rows += n

    with scope("gather_early"):
        tables((HERE, ON, BACK))
        for i, j in early:
            gather(i, j, sent.at[i, j], end=FAR)
            start(*(("s", i, j, k) for k in range(free)))
    with scope("xx_wait"):
        arrived("xx", xg.at[FAR])
        arrived("mm", mg.at[FAR, FAR])
    with scope("tables"):
        tables(range(OFFSETS))
    for i, j in early:
        with scope("gather_far"):
            gather_far(i, j, sent.at[i, j])
        start(*(("s", i, j, k) for k in range(free, len(spans))))
    with scope("gather"):
        gather(HERE, OTHER, sent.at[HERE, OTHER])
        start(("s", HERE, OTHER))
        gather(HERE, SAME, z.at[SAME, HERE])
        gather(ON, OTHER, sent.at[ON, OTHER])
        gather(BACK, OTHER, sent.at[BACK, OTHER])

    with scope("wait_here"):
        arrived("s_here", z.at[OTHER, HERE])
    with scope("ffn_here_up"):
        expert_ups(1, (SAME, HERE), (OTHER, HERE))
    with scope("wait_f"):
        arrived("fwd", fwd)
        start(("z", FAR, SAME), ("z", FAR, OTHER))
    with scope("ffn_here_down"):
        expert_downs(1, r.at[index[HERE, SAME]], z.at[OTHER, HERE])
    start(("s", ON, OTHER), ("s", BACK, OTHER))
    start(("r", HERE, OTHER))
    with scope("weigh"):
        gone("x", xg.at[pl.ds(0, 3)])
        for s in range(OFFSETS):
            token = lax.broadcasted_iota(jnp.int32, (tokens, total), 0).astype(F32) + 1.0
            xg[s] = jnp.where(token == table(s), table(s, 1), 0.0).astype(BF16)
    with scope("wait_same"):
        arrived(("s", SAME), z.at[SAME, pl.ds(ON, 2)])
    with scope("ffn_same"):
        expert_ups(2, (SAME, ON), (SAME, BACK))
        expert_downs(2, z.at[SAME, ON], z.at[SAME, BACK])
    start(("r", ON, SAME), ("r", BACK, SAME))
    with scope("wait_far"):
        arrived("z_far", z.at[:, FAR])
    with scope("ffn_far"):
        expert_ups(3, (SAME, FAR), (OTHER, FAR))
        for v in range(2):
            expert_downs(3, z.at[SAME, FAR], z.at[OTHER, FAR], v * n_down // 4, (v + 1) * n_down // 4)
            start(("g", SAME, v), ("g", OTHER, v))
    with scope("wait_other"):
        arrived(("s", OTHER), z.at[OTHER, pl.ds(ON, 2)])
    with scope("ffn_other"):
        expert_ups(4, (OTHER, ON), (OTHER, BACK))
        for v in range(2):
            expert_downs(4, z.at[OTHER, ON], z.at[OTHER, BACK], v * n_down // 4, (v + 1) * n_down // 4)
            if v == 0:
                start(("r", ON, OTHER, v), ("r", BACK, OTHER, v))
    with scope("wait_g"):
        for v, cols in enumerate(sides):
            arrived(("g", v), fwdb.at[:, :, cols])
            start(("r", FAR, SAME, v), ("r", FAR, OTHER, v))
            if v == 0:
                start(("r", ON, OTHER, 1), ("r", BACK, OTHER, 1))

    def add_up(s, v, first=0, end=units):
        cols = sides[v]
        these = pl.ds(first * full, (end - first) * full)
        return dot(xg[s, :, these], r[first:end, :, cols].reshape((end - first) * full, d // 2))

    with scope("wait_r_same"):
        arrived("r", r.at[near_units, body])
    def sum_far(v):
        cols = sides[v]
        with scope("wait_r_other"):
            arrived(("r", OTHER, v), r.at[other_units, body, cols])
        with scope("sum_far_early"):
            o = add_up(FAR, v, end=index[FAR, SAME])
            near[0, :, cols] = o[:half]
            near[1, :, cols] = o[half:]
        with scope("wait_r_far"):
            arrived(("r", FAR, v), r.at[far_units, body, cols])
        with scope("sum_far"):
            o = add_up(FAR, v, first=index[FAR, SAME])
            part[2, lo, cols] = (near[0, :, cols] + o[:half]).astype(BF16)
            part[2, hi, cols] = (near[1, :, cols] + o[half:]).astype(BF16)
        start(("pp", 0, v), ("pp", 1, v))

    def sum_near(v):
        cols = sides[v]
        with scope("sum_near"):
            o = add_up(BACK, v)
            near[0, :, cols] = o[:half]
            part[0, hi, cols] = o[half:].astype(BF16)
            start(("p", 0, 0, v))
            o = add_up(ON, v)
            near[1, :, cols] = o[half:]
            part[1, lo, cols] = o[:half].astype(BF16)
            start(("p", 1, 0, v))

    def sum_own(v):
        with scope("sum_own"):
            ysh[:, sides[v]] = ysh[:, sides[v]] + add_up(HERE, v)

    def pass_on(v):
        cols = sides[v]
        with scope("wait_pp"):
            arrived(("pp", v), rfar.at[:, :, cols])
            for k, first in ((0, lo), (1, hi)):
                part[k, first, cols] = (near[k, :, cols] + rfar[k, :, cols].astype(F32)).astype(BF16)
                start(("p", k, 1, v))

    sum_far(0)
    sum_near(0)
    sum_own(0)
    sum_far(1)
    pass_on(0)
    sum_near(1)
    sum_own(1)
    pass_on(1)
    for v, cols in enumerate(sides):
        with scope("wait_p"):
            arrived(("p", v), rn.at[:, :, cols])
        with scope("leave"):
            y = ysh[:, cols] + (rn[0, :, cols].astype(F32) + rn[1, :, cols].astype(F32))
            y_ref[:, cols] = y.astype(y_ref.dtype)
    with scope("end"):
        gone("m", mg.at[HERE])
        gone("s_here", sent.at[HERE, OTHER])
        gone("s", sent.at[pl.ds(ON, 3)])
        gone("fwd", fwd)
        gone(("z", SAME), z.at[SAME, pl.ds(ON, 3)])
        gone(("z", OTHER), z.at[OTHER])
        gone("fwdb", fwdb)
        gone("part", part)


def solution(mesh):
    side = math.isqrt(mesh.shape["ep"] // 2)
    assert side == OFFSETS

    def local(x, expert, slot, gate, w_gate, w_up, w_down, s_gate, s_up, s_down):
        tokens, d = x.shape[2:]
        top = expert.shape[3]
        per, _, ff = w_gate.shape
        experts = per * mesh.shape["ep"]
        slots = 5 * tokens * top // (4 * experts)
        unit = per * OFFSETS * slots
        full = unit + (-unit) % LANE
        half, units = tokens // 2, len(UNITS)
        choices = (v.transpose(0, 3, 1, 2).reshape(top, 1, tokens) for v in (expert, slot, gate))
        anywhere = pl.BlockSpec(memory_space=pl.ANY)
        y = pl.pallas_call(
            functools.partial(kernel, side, slots),
            out_shape=pltpu.VMEM((tokens, d), x.dtype),
            in_specs=[anywhere] * 10,
            out_specs=pl.BlockSpec(memory_space=pltpu.VMEM),
            scratch_shapes=[
                *(pltpu.VMEM((top, 1, tokens), v.dtype) for v in (expert, slot, gate)),
                pltpu.VMEM((OFFSETS, tokens, d), BF16),
                pltpu.VMEM((OFFSETS, OFFSETS, 2, units * full), F32),
                pltpu.VMEM((units * full, 2 * OFFSETS), F32),
                pltpu.VMEM((unit, OFFSETS * tokens), BF16),
                pltpu.VMEM((OFFSETS, 2, unit, d), BF16),
                pltpu.VMEM((2, unit, d), BF16),
                pltpu.VMEM((2, OFFSETS, unit, d), BF16),
                pltpu.VMEM((units, full, d), BF16),
                pltpu.VMEM((2, unit, d), BF16),
                pltpu.VMEM((per, 2 * (unit // per + 8), ff), BF16),
                pltpu.VMEM((BUFFERS, per, d, WIDE), BF16),
                pltpu.VMEM((3, tokens, d), BF16),
                pltpu.VMEM((2, half, d), F32),
                pltpu.VMEM((2, half, d), BF16),
                pltpu.VMEM((2, tokens, d), BF16),
                pltpu.VMEM((tokens, d), F32),
                pltpu.SemaphoreType.DMA((4,)),
                pltpu.SemaphoreType.DMA((BUFFERS,)),
                pltpu.SemaphoreType.DMA((SENDS,)),
                pltpu.SemaphoreType.DMA((LANDINGS,)),
            ],
            compiler_params=pltpu.CompilerParams(
                collective_id=0, has_side_effects=True, vmem_limit_bytes=64_500_000),
            name="moe",
        )(x.reshape(tokens, d), *choices, w_gate, w_up, w_down, s_gate, s_up, s_down)
        return y.reshape(x.shape)

    spread, held, whole = P("dp", "ep", None, None), P("ep", None, None), P(None, None)
    return jax.shard_map(
        local, mesh=mesh, in_specs=(spread,) * 4 + (held,) * 3 + (whole,) * 3, out_specs=spread, check_vma=False)
```
